32 devices in a mesh: group: 2 (over core), dom: 16 (over z, y, x).
Axes of the slice: x: 2, y: 2, z: 4, core: 2. Of those that a mesh axis runs over, the one named last changes fastest.
Arguments:
- nodes: bfloat16 [2, 16384, 512], P('group', 'dom'), may hold values from -6 to 6
- edges: bfloat16 [2, 32768, 512], P('group', 'dom'), may hold values from -6 to 6
- node_cotangent: bfloat16 [2, 16384, 512], P('group', 'dom'), may hold values from -6 to 6
- edge_cotangent: bfloat16 [2, 32768, 512], P('group', 'dom'), may hold values from -6 to 6
- senders: int32 [2, 32768], P('group', 'dom'), may hold values from 0 to 1151, as said below
- receivers: int32 [2, 32768], P('group', 'dom'), may hold values from 0 to 1023
- send_rows: int32 [2, 256, 8], P('group', 'dom'), may hold values from 0 to 1023
- edge_in: bfloat16 [1536, 512], replicated, may hold values from -0.15625 to 0.15625
- edge_out: bfloat16 [512, 512], replicated, may hold values from -0.25 to 0.25
- edge_gain: float32 [512], replicated, may hold values from 0.1 to 1.9
- node_in: bfloat16 [1024, 512], replicated, may hold values from -0.1875 to 0.1875
- node_out: bfloat16 [512, 512], replicated, may hold values from -0.25 to 0.25
- node_gain: float32 [512], replicated, may hold values from 0.1 to 1.9
Outputs:
- grad_edges: bfloat16 [2, 32768, 512], P('group', 'dom')
- grad_nodes: bfloat16 [2, 16384, 512], P('group', 'dom')
- grad_edge_in: float32 [1536, 512], P('dom')
- grad_edge_out: float32 [512, 512], P('dom')
- grad_node_in: float32 [1024, 512], P('dom')
- grad_node_out: float32 [512, 512], P('dom')
- grad_edge_gain: float32 [512], P('dom')
- grad_node_gain: float32 [512], P('dom')
The draws below stay inside these ranges and needn't reach their ends.
Inputs may be any that keep to these rules, and one draw needn't show every extreme that they name: `senders`: an id below 1024 is a row of the edge's own partition; an id 1024 + p * 8 + s is slot s of the list partition p of the same graph sends to the edge's partition. The slots read from one peer lie below a count of that edge's partition and peer, and on every partition some peer's slot 7 is read.
All inputs are finite; a program needn't handle non-finite values.
Results may differ from the reference program's by a relative error of at most 0.019.
Values may be sent and summed in bfloat16 or wider, within the bound.
A program may use at most 128 MiB of HBM per device.

```python
import jax
import jax.numpy as jnp
from jax import lax

W = 512
NODE_DEV = 1024
EDGE_DEV = 2048
CAP = 8
DOMAINS = 16
GRAPHS = 2
NODES = 16384
EDGES = 32768


def draw_senders(key, part):
    keys = jax.random.split(jax.random.fold_in(key, 7), 6)
    used = jax.random.randint(keys[0], (GRAPHS, DOMAINS, DOMAINS), 1, CAP + 1)
    full_peer = jax.random.randint(keys[1], (GRAPHS, DOMAINS), 0, DOMAINS)
    peer_iota = jnp.arange(DOMAINS, dtype=jnp.int32)[None, None, :]
    used = jnp.where(peer_iota == full_peer[:, :, None], CAP, used)
    peer = jax.random.randint(keys[2], (GRAPHS, DOMAINS, EDGE_DEV), 0, DOMAINS)
    noise = jax.random.randint(keys[3], (GRAPHS, DOMAINS, EDGE_DEV), 0, 1 << 20)
    limit = jnp.take_along_axis(used, peer, axis=2)
    slot = noise % limit
    halo_ids = NODE_DEV + peer * CAP + slot
    local_ids = jax.random.randint(keys[4], (GRAPHS, DOMAINS, EDGE_DEV), 0, NODE_DEV)
    picker = jax.random.randint(keys[5], (GRAPHS, DOMAINS, EDGE_DEV), 0, 2)
    result = jnp.where(picker == 0, local_ids, halo_ids)
    result = result.at[:, :, 0].set(NODE_DEV + full_peer * CAP + CAP - 1)
    return result.reshape(GRAPHS, DOMAINS * EDGE_DEV).astype(jnp.int32)


def place_ends(values, rng, smallest, largest):
    index_at = [jax.random.randint(jax.random.fold_in(rng, axis), (), 0, length) for axis, length in enumerate(values.shape)]
    main_axis = values.shape.index(max(values.shape))
    neighbour = index_at[:main_axis] + [(index_at[main_axis] + 1) % values.shape[main_axis]] + index_at[main_axis + 1:]
    return values.at[tuple(index_at)].set(smallest).at[tuple(neighbour)].set(largest)


def shard_levels(key, shape, pieces, low, high):
    def one(position, blocks):
        steps = jax.random.uniform(jax.random.fold_in(jax.random.fold_in(key, 6), position), (blocks,), jnp.float32, low / len(pieces), high / len(pieces))
        return jnp.repeat(jnp.exp(steps), shape[position] // blocks).reshape((-1,) + (1,) * (len(shape) - position - 1))

    level = one(*pieces[0])
    for cut in pieces[1:]:
        level = level * one(*cut)
    return level


def gaussian(stream_key, extent, spread, reach, cuts=(), kind=jnp.bfloat16):
    array = jax.random.normal(stream_key, extent, jnp.float32) * spread
    if len(cuts) > 0:
        array = shard_levels(stream_key, extent, cuts, -0.22, 0.18) * array
    return jnp.clip(array, min=-reach, max=reach).astype(kind)


def setup_inputs(seed: int = 0) -> dict:
    streams_of = jax.random.split(jax.random.key(seed), 14)
    return {
        "nodes": gaussian(streams_of[0], (GRAPHS, NODES, W), 1.0, 6.0, ((0, 2), (1, 16))),
        "edges": gaussian(streams_of[1], (GRAPHS, EDGES, W), 1.0, 6.0, ((0, 2), (1, 16))),
        "node_cotangent": gaussian(streams_of[2], (GRAPHS, NODES, W), 1.0, 6.0, ((0, 2), (1, 16))),
        "edge_cotangent": gaussian(streams_of[3], (GRAPHS, EDGES, W), 1.0, 6.0, ((0, 2), (1, 16))),
        "senders": draw_senders(jax.random.fold_in(streams_of[13], 71), 0),
        "receivers": place_ends(jax.random.randint(streams_of[5], (GRAPHS, EDGES), 0, NODE_DEV), jax.random.fold_in(streams_of[5], 1), 0, NODE_DEV - 1).astype(jnp.int32),
        "send_rows": place_ends(jax.random.randint(streams_of[6], (GRAPHS, DOMAINS * DOMAINS, CAP), 0, NODE_DEV), jax.random.fold_in(streams_of[6], 1), 0, NODE_DEV - 1).astype(jnp.int32),
        "edge_in": gaussian(streams_of[7], (3 * W, W), (3 * W) ** -0.5, 0.15625),
        "edge_out": gaussian(streams_of[8], (W, W), W ** -0.5, 0.25),
        "edge_gain": jnp.clip(1.0 + 0.18 * jax.random.normal(streams_of[9], (W,), jnp.float32), 0.1, 1.9),
        "node_in": gaussian(streams_of[10], (2 * W, W), (2 * W) ** -0.5, 0.1875),
        "node_out": gaussian(streams_of[11], (W, W), W ** -0.5, 0.25),
        "node_gain": jnp.clip(1.0 + 0.18 * jax.random.normal(streams_of[12], (W,), jnp.float32), 0.1, 1.9),
    }


def swish(value):
    return value * jax.nn.sigmoid(value)

def swish_slope(value):
    logistic = jax.nn.sigmoid(value)
    return logistic * (1.0 + value * (1.0 - logistic))

def normalize(hidden):
    centre = hidden - lax.optimization_barrier(jnp.mean(hidden, axis=-1, keepdims=True))
    inverse = lax.rsqrt(lax.optimization_barrier(jnp.mean(centre * centre, axis=-1, keepdims=True)) + 1e-05)
    return (centre * inverse, inverse)

def norm_back(upstream, gain, normed, inverse):
    scaled = upstream * gain
    return inverse * (scaled - lax.optimization_barrier(jnp.mean(scaled, axis=-1, keepdims=True)) - normed * lax.optimization_barrier(jnp.mean(scaled * normed, axis=-1, keepdims=True)))

def one_graph(node_rows, edge_rows, node_cot, edge_cot, send_ids, recv_ids, lists, edge_in, edge_out, edge_gain, node_in, node_out, node_gain):
    edge_index = jnp.arange(EDGES, dtype=jnp.int32)
    owner = edge_index // EDGE_DEV
    recv_node = owner * NODE_DEV + recv_ids
    lists = lists.reshape(DOMAINS, DOMAINS, CAP)
    halo_pos = jnp.maximum(send_ids - NODE_DEV, 0)
    peer = halo_pos // CAP
    slot = halo_pos % CAP
    remote_row = lists[peer, owner, slot]
    send_node = jnp.where(send_ids < NODE_DEV, owner * NODE_DEV + send_ids, peer * NODE_DEV + remote_row)
    edge_input = jnp.concatenate([edge_rows, node_rows[send_node], node_rows[recv_node]], axis=1)
    edge_pre = jnp.dot(edge_input, edge_in, preferred_element_type=jnp.float32)
    edge_act = swish(edge_pre).astype(jnp.bfloat16)
    edge_post = jnp.dot(edge_act, edge_out, preferred_element_type=jnp.float32)
    edge_hat, edge_inv = normalize(edge_post)
    update = (edge_hat * edge_gain).astype(jnp.bfloat16)
    gathered = jax.ops.segment_sum(update.astype(jnp.float32), recv_node, NODES).astype(jnp.bfloat16)
    node_input = jnp.concatenate([node_rows, gathered], axis=1)
    node_pre = jnp.dot(node_input, node_in, preferred_element_type=jnp.float32)
    node_act = swish(node_pre).astype(jnp.bfloat16)
    node_post = jnp.dot(node_act, node_out, preferred_element_type=jnp.float32)
    node_hat, node_inv = normalize(node_post)
    node_upstream = node_cot.astype(jnp.float32)
    node_gain_grad = lax.optimization_barrier(jnp.sum(node_upstream * node_hat, axis=0))
    node_post_grad = norm_back(node_upstream, node_gain, node_hat, node_inv).astype(jnp.bfloat16)
    node_out_grad = jnp.dot(node_act.T, node_post_grad, preferred_element_type=jnp.float32)
    node_act_grad = jnp.dot(node_post_grad, node_out.T, preferred_element_type=jnp.float32)
    node_pre_grad = (node_act_grad * swish_slope(node_pre)).astype(jnp.bfloat16)
    node_in_grad = jnp.dot(node_input.T, node_pre_grad, preferred_element_type=jnp.float32)
    node_input_grad = jnp.dot(node_pre_grad, node_in.T, preferred_element_type=jnp.float32)
    gathered_grad = node_input_grad[:, W:].astype(jnp.bfloat16)
    update_grad = edge_cot.astype(jnp.float32) + gathered_grad[recv_node].astype(jnp.float32)
    edge_gain_grad = lax.optimization_barrier(jnp.sum(update_grad * edge_hat, axis=0))
    edge_post_grad = norm_back(update_grad, edge_gain, edge_hat, edge_inv).astype(jnp.bfloat16)
    edge_out_grad = jnp.dot(edge_act.T, edge_post_grad, preferred_element_type=jnp.float32)
    edge_act_grad = jnp.dot(edge_post_grad, edge_out.T, preferred_element_type=jnp.float32)
    edge_pre_grad = (edge_act_grad * swish_slope(edge_pre)).astype(jnp.bfloat16)
    edge_in_grad = jnp.dot(edge_input.T, edge_pre_grad, preferred_element_type=jnp.float32)
    edge_input_grad = jnp.dot(edge_pre_grad, edge_in.T, preferred_element_type=jnp.float32)
    grad_edges = (edge_cot.astype(jnp.float32) + edge_input_grad[:, :W]).astype(jnp.bfloat16)
    node_total = node_upstream + node_input_grad[:, :W]
    node_total = node_total + jax.ops.segment_sum(edge_input_grad[:, W:2 * W], send_node, NODES)
    node_total = node_total + jax.ops.segment_sum(edge_input_grad[:, 2 * W:], recv_node, NODES)
    grad_nodes = node_total.astype(jnp.bfloat16)
    return (grad_edges, grad_nodes, (edge_in_grad, edge_out_grad, node_in_grad, node_out_grad, edge_gain_grad, node_gain_grad))

def reference(nodes, edges, node_cotangent, edge_cotangent, senders, receivers, send_rows, edge_in, edge_out, edge_gain, node_in, node_out, node_gain):
    edge_list = []
    node_list = []
    totals = None
    for graph in range(GRAPHS):
        grad_e, grad_n, parts = one_graph(nodes[graph], edges[graph], node_cotangent[graph], edge_cotangent[graph], senders[graph], receivers[graph], send_rows[graph], edge_in, edge_out, edge_gain, node_in, node_out, node_gain)
        edge_list.append(grad_e)
        node_list.append(grad_n)
        if totals is None:
            totals = parts
        else:
            totals = tuple((first + second for first, second in zip(totals, parts)))
    return (jnp.stack(edge_list), jnp.stack(node_list), totals[0], totals[1], totals[2], totals[3], totals[4], totals[5])
```

```python
import functools

import jax
import jax.numpy as jnp
from jax import lax
from jax.experimental import pallas as pl
from jax.experimental.pallas import tpu as pltpu
from jax.sharding import PartitionSpec as P

MESH = pl.DeviceIdType.MESH
F32 = jnp.float32
BF16 = jnp.bfloat16
I32 = jnp.int32
LANES = 128


def dot(first, second):
    return jnp.dot(first, second, preferred_element_type=F32)


def dot_tn(first, second):
    return lax.dot_general(first, second, (((0,), (0,)), ((), ())), preferred_element_type=F32)


def dot_nt(first, second):
    return lax.dot_general(first, second, (((1,), (1,)), ((), ())), preferred_element_type=F32)


def normalize(hidden):
    centre = hidden - jnp.mean(hidden, axis=-1, keepdims=True)
    inverse = lax.rsqrt(jnp.mean(centre * centre, axis=-1, keepdims=True) + 1e-05)
    return centre * inverse, inverse


def norm_back(upstream, gain, normed, inverse):
    scaled = upstream * gain
    return inverse * (
        scaled
        - jnp.mean(scaled, axis=-1, keepdims=True)
        - normed * jnp.mean(scaled * normed, axis=-1, keepdims=True)
    )


def swish_pair(value):
    logistic = jax.nn.sigmoid(value)
    return value * logistic, logistic * (1.0 + value * (1.0 - logistic))


def hot(mask):
    return jnp.where(mask, 1.0, 0.0).astype(BF16)


def pick_rows(column, base, count):
    lane = lax.broadcasted_iota(I32, column.shape, 1)
    return jnp.concatenate(
        [hot(column == lane + (base + block)) for block in range(0, count, LANES)], axis=1
    )


def pick_columns(row, base, count):
    index = lax.broadcasted_iota(I32, (count, row.shape[1]), 0) + base
    return hot(index == row)


def fold(value):
    return jnp.sum(value.reshape(value.shape[0] // 8, 8, value.shape[1]), axis=0)


def tile_of(count, sizes):
    return next(size for size in sizes if count % size == 0)


class Chunk:
    def __init__(self, env, mat, out, start, wide, refs):
        self.env, self.mat, self.out, self.start, self.wide = env, mat, out, start, wide
        (
            self.from_graph, self.sum_graph, self.from_plane, self.sum_plane, self.from_layer,
            self.total, self.from_other, self.sem,
        ) = refs
        self.slot = 0

    def send(self, src, dst, device):
        slot = self.slot
        self.slot += 1
        return self.env.send(src, dst, self.sem.at[0, slot], self.sem.at[1, slot], device)

    def columns(self, group):
        return pl.ds(pl.multiple_of(self.start + group * self.wide, LANES), self.wide)

    def graph(self):
        env = self.env
        self.graph_copy = self.send(
            self.mat.at[:, self.columns(env.other)], self.from_graph, (env.other, env.dom)
        )

    def planes(self):
        env = self.env
        self.graph_copy.wait_recv()
        value = self.mat[:, self.columns(env.group)].astype(F32) + self.from_graph[...].astype(F32)
        self.sum_graph[...] = value.astype(BF16).reshape(self.sum_graph.shape)
        self.rows = self.from_layer.shape[1]
        self.plane_copies = []
        for step in range(1, env.planes):
            target = lax.rem(env.plane + step, env.planes)
            self.plane_copies.append(
                self.send(
                    self.sum_graph.at[:, target],
                    self.from_plane.at[step - 1],
                    (env.group, env.layer * env.planes + target),
                )
            )

    def layers(self):
        env = self.env
        value = self.sum_graph[:, env.plane].astype(F32)
        for step in range(1, env.planes):
            self.plane_copies[step - 1].wait_recv()
            value = value + self.from_plane[step - 1].astype(F32)
        self.sum_plane[...] = value.astype(BF16)
        self.layer_copies = []
        for step in range(1, env.layers):
            target = lax.rem(env.layer + step, env.layers)
            self.layer_copies.append(
                self.send(
                    self.sum_plane.at[target],
                    self.from_layer.at[step - 1],
                    (env.group, target * env.planes + env.plane),
                )
            )

    def finish(self):
        env = self.env
        value = self.sum_plane[env.layer].astype(F32)
        for step in range(1, env.layers):
            self.layer_copies[step - 1].wait_recv()
            value = value + self.from_layer[step - 1].astype(F32)
        short = value.astype(BF16)
        self.total[...] = short
        self.other_copy = self.send(self.total, self.from_other, (env.other, env.dom))
        self.out[:, self.columns(env.group)] = short.astype(F32)

    def place(self):
        self.other_copy.wait_recv()
        self.out[:, self.columns(self.env.other)] = self.from_other[...].astype(F32)


class Env:
    pass


def layer_kernel(shape, *refs):
    node_count, edge_count, width, domains, slots, planes, layers, plan = shape
    halo = domains * slots
    rows_all = node_count + halo
    inputs, refs = refs[:13], refs[13:]
    (edges_out, nodes_out, ein_out, eout_out, nin_out, nout_out, gain_out), refs = refs[:7], refs[7:]
    loaded, refs = refs[:13], refs[13:]
    (
        nodes, edges, ncot, ecot, send_row, recv_row, list_in, ein, eout, egain, nin, nout, ngain,
    ) = loaded
    (
        send_col, recv_col, list_col, outgoing, arrived, from_table, to_table, halo_table,
        edge_pre, edge_slope, edge_act, edge_hat, edge_inv, edge_mid, edge_grad,
        gathered, node_act, node_mid, node_grad, gathered_grad, sums_from, sums_to, returning, returned,
        ein_grad, eout_grad, nin_grad, nout_grad,
        gains, gain_graph, gain_mine, gain_plane, gain_mid, gain_layer,
        load_sem, halo_sem, back_sem, gain_sem,
    ), refs = refs[:38], refs[38:]

    env = Env()
    env.group = lax.axis_index("group")
    env.dom = lax.axis_index("dom")
    env.other = 1 - env.group
    env.planes, env.layers = planes, layers
    env.layer = env.dom // planes
    env.plane = lax.rem(env.dom, planes)
    sent = []

    def send(src, dst, send_sem, recv_sem, device):
        copy = pltpu.make_async_remote_copy(
            src_ref=src, dst_ref=dst, send_sem=send_sem, recv_sem=recv_sem,
            device_id=device, device_id_type=MESH,
        )
        copy.start()
        sent.append(copy)
        return copy

    env.send = send

    def peer(step):
        return lax.rem(env.dom + step, domains)

    loads = [
        pltpu.make_async_copy(src, dst, load_sem.at[index])
        for index, (src, dst) in enumerate(zip(inputs, loaded))
    ]
    NODES, EDGES, NCOT, ECOT, SEND, RECV, LIST, EIN, EOUT, EGAIN, NIN, NOUT, NGAIN = range(13)
    for index in (LIST, NODES, SEND, RECV, EIN, EDGES, EOUT, EGAIN, NIN, NOUT, NGAIN, NCOT, ECOT):
        loads[index].start()

    barrier = pltpu.get_barrier_semaphore()
    pl.semaphore_signal(barrier, inc=1, device_id=(env.other, env.dom), device_id_type=MESH)
    for step in range(1, domains):
        pl.semaphore_signal(barrier, inc=1, device_id=(env.group, peer(step)), device_id_type=MESH)

    loads[LIST].wait()
    for index in range(domains):
        list_col[index * slots : (index + 1) * slots, :] = jnp.broadcast_to(
            list_in[:, index : index + 1], (slots, LANES)
        )
    loads[NODES].wait()
    outgoing[...] = (
        dot(pick_rows(list_col[...], 0, node_count), nodes[...])
        .astype(BF16)
        .reshape(domains, slots, width)
    )
    pl.semaphore_wait(barrier, domains)
    halo_copies = [
        send(
            outgoing.at[peer(step)],
            arrived.at[env.dom],
            halo_sem.at[0, step - 1],
            halo_sem.at[1, step - 1],
            (env.group, peer(step)),
        )
        for step in range(1, domains)
    ]
    arrived[env.dom] = outgoing[env.dom]

    loads[SEND].wait()
    loads[RECV].wait()

    @pl.loop(0, edge_count // LANES)
    def _(index):
        place = pl.ds(pl.multiple_of(index * LANES, LANES), LANES)
        send_col[place, :] = jnp.transpose(jnp.broadcast_to(send_row[:, place], (LANES, LANES)))
        recv_col[place, :] = jnp.transpose(jnp.broadcast_to(recv_row[:, place], (LANES, LANES)))

    loads[EIN].wait()
    own_w = slice(0, width)
    from_w = slice(width, 2 * width)
    to_w = slice(2 * width, 3 * width)
    step_n = tile_of(node_count, (512, 256, 128))

    @pl.loop(0, node_count // step_n)
    def _(index):
        place = pl.ds(pl.multiple_of(index * step_n, step_n), step_n)
        from_table[place, :] = dot(nodes[place, :], ein[from_w, :]).astype(BF16)
        to_table[place, :] = dot(nodes[place, :], ein[to_w, :]).astype(BF16)

    loads[EDGES].wait()
    step_e = tile_of(edge_count, (256, 128))

    @pl.loop(0, edge_count // step_e)
    def _(index):
        place = pl.ds(pl.multiple_of(index * step_e, step_e), step_e)
        edge_pre[place, :] = (
            dot(edges[place, :], ein[own_w, :])
            + dot(pick_rows(send_col[place, :], 0, node_count), from_table[...])
            + dot(pick_rows(recv_col[place, :], 0, node_count), to_table[...])
        )

    loads[EOUT].wait()
    loads[EGAIN].wait()
    for copy in halo_copies:
        copy.wait_recv()
    halo_table[...] = dot(arrived[...].reshape(halo, width), ein[from_w, :]).astype(BF16)

    @pl.loop(0, edge_count // step_e)
    def _(index):
        place = pl.ds(pl.multiple_of(index * step_e, step_e), step_e)
        value = edge_pre[place, :] + dot(
            pick_rows(send_col[place, :], node_count, halo), halo_table[...]
        )
        act, slope = swish_pair(value)
        act = act.astype(BF16)
        edge_act[place, :] = act
        edge_slope[place, :] = slope
        normed, inverse = normalize(dot(act, eout[...]))
        edge_hat[place, :] = normed
        edge_inv[place, :] = jnp.broadcast_to(inverse, (step_e, LANES))
        edge_mid[place, :] = (normed * egain[...]).astype(BF16)

    for index in (NIN, NOUT, NGAIN, NCOT):
        loads[index].wait()
    near = slice(0, width)
    far = slice(width, 2 * width)
    gains[...] = jnp.zeros_like(gains)
    step_v = tile_of(node_count, (256, 128))

    @pl.loop(0, node_count // step_v)
    def _(index):
        start = pl.multiple_of(index * step_v, step_v)
        place = pl.ds(start, step_v)
        got = dot(pick_columns(recv_row[...], start, step_v), edge_mid[...]).astype(BF16)
        gathered[place, :] = got
        act, slope = swish_pair(dot(nodes[place, :], nin[near, :]) + dot(got, nin[far, :]))
        act = act.astype(BF16)
        node_act[place, :] = act
        normed, inverse = normalize(dot(act, nout[...]))
        upstream = ncot[place, :].astype(F32)
        gains[8:16, :] += fold(upstream * normed)
        post = norm_back(upstream, ngain[...], normed, inverse).astype(BF16)
        node_mid[place, :] = post
        grad = (dot_nt(post, nout[...]) * slope).astype(BF16)
        node_grad[place, :] = grad
        gathered_grad[place, :] = dot_nt(grad, nin[far, :]).astype(BF16)

    chunks = {}
    mats = {"ein": ein_grad, "eout": eout_grad, "nin": nin_grad, "nout": nout_grad}
    outs = {"ein": ein_out, "eout": eout_out, "nin": nin_out, "nout": nout_out}
    for index, (name, start, wide) in enumerate(plan):
        chunks[name, start] = Chunk(
            env, mats[name], outs[name], start, wide, refs[index * 8 : (index + 1) * 8]
        )
    half = width // 2
    nout_c, nin_c, eout_c = chunks["nout", 0], chunks["nin", 0], chunks["eout", 0]
    ein_c = (chunks["ein", 0], chunks["ein", half])

    nout_grad[...] = dot_tn(node_act[...], node_mid[...]).astype(BF16)
    nout_c.graph()
    nin_grad[near, :] = dot_tn(nodes[...], node_grad[...]).astype(BF16)
    nin_grad[far, :] = dot_tn(gathered[...], node_grad[...]).astype(BF16)
    nin_c.graph()

    loads[ECOT].wait()

    @pl.loop(0, edge_count // step_e)
    def _(index):
        place = pl.ds(pl.multiple_of(index * step_e, step_e), step_e)
        upstream = ecot[place, :].astype(F32) + dot(
            pick_rows(recv_col[place, :], 0, node_count), gathered_grad[...]
        )
        normed = edge_hat[place, :]
        gains[0:8, :] += fold(upstream * normed)
        edge_mid[place, :] = norm_back(
            upstream, egain[...], normed, edge_inv[place, 0:1]
        ).astype(BF16)

    nout_c.planes()
    nin_c.planes()
    gains[0:1, :] = jnp.sum(gains[0:8, :], axis=0, keepdims=True)
    gains[1:2, :] = jnp.sum(gains[8:16, :], axis=0, keepdims=True)
    gain_graph_copy = send(
        gains.at[0:8], gain_graph, gain_sem.at[0, 0], gain_sem.at[1, 0], (env.other, env.dom)
    )

    eout_grad[...] = dot_tn(edge_act[...], edge_mid[...]).astype(BF16)
    eout_c.graph()

    gain_graph_copy.wait_recv()
    gain_mine[...] = gains[0:8, :] + gain_graph[...]
    gain_copies = [
        send(
            gain_mine, gain_plane.at[step - 1], gain_sem.at[0, step], gain_sem.at[1, step],
            (env.group, env.layer * planes + lax.rem(env.plane + step, planes)),
        )
        for step in range(1, planes)
    ]

    @pl.loop(0, edge_count // step_e)
    def _(index):
        place = pl.ds(pl.multiple_of(index * step_e, step_e), step_e)
        edge_grad[place, :] = (
            dot_nt(edge_mid[place, :], eout[...]) * edge_slope[place, :]
        ).astype(BF16)

    nout_c.layers()
    nin_c.layers()
    eout_c.planes()
    total = gain_mine[...]
    for step in range(1, planes):
        gain_copies[step - 1].wait_recv()
        total = total + gain_plane[step - 1]
    gain_mid[...] = total
    gain_copies = [
        send(
            gain_mid, gain_layer.at[step - 1],
            gain_sem.at[0, planes + step - 1], gain_sem.at[1, planes + step - 1],
            (env.group, lax.rem(env.layer + step, layers) * planes + env.plane),
        )
        for step in range(1, layers)
    ]

    step_s = tile_of(rows_all, (384, 256, 128))
    step_t = tile_of(node_count, (256, 128))

    def scatter_from(columns):
        @pl.loop(0, rows_all // step_s)
        def _(index):
            start = pl.multiple_of(index * step_s, LANES)
            sums_from[pl.ds(start, step_s), columns] = dot(
                pick_columns(send_row[...], start, step_s), edge_grad[:, columns]
            ).astype(BF16)

    def scatter_to(columns):
        @pl.loop(0, node_count // step_t)
        def _(index):
            start = pl.multiple_of(index * step_t, step_t)
            sums_to[pl.ds(start, step_t), columns] = dot(
                pick_columns(recv_row[...], start, step_t), edge_grad[:, columns]
            ).astype(BF16)

    def edge_in_grads(columns):
        ein_grad[own_w, columns] = dot_tn(edges[...], edge_grad[:, columns]).astype(BF16)
        ein_grad[from_w, columns] = (
            dot_tn(nodes[...], sums_from[0:node_count, columns])
            + dot_tn(arrived[...].reshape(halo, width), sums_from[node_count:rows_all, columns])
        ).astype(BF16)
        ein_grad[to_w, columns] = dot_tn(nodes[...], sums_to[:, columns]).astype(BF16)

    first, second = slice(0, half), slice(half, width)
    scatter_from(first)
    scatter_to(first)
    edge_in_grads(first)
    ein_c[0].graph()
    nout_c.finish()
    nin_c.finish()
    eout_c.layers()

    scatter_from(second)
    returning[...] = (
        dot_nt(sums_from[node_count:rows_all, :], ein[from_w, :])
        .astype(BF16)
        .reshape(domains, slots, width)
    )
    back_copies = [
        send(
            returning.at[peer(step)],
            returned.at[env.dom],
            back_sem.at[0, step - 1],
            back_sem.at[1, step - 1],
            (env.group, peer(step)),
        )
        for step in range(1, domains)
    ]
    returned[env.dom] = returning[env.dom]
    ein_c[0].planes()
    scatter_to(second)
    edge_in_grads(second)
    ein_c[1].graph()
    nout_c.place()
    nin_c.place()
    eout_c.finish()
    ein_c[0].layers()

    total = gain_mid[...]
    for step in range(1, layers):
        gain_copies[step - 1].wait_recv()
        total = total + gain_layer[step - 1]
    gain_out[...] = total

    def edge_tail(begin, end):
        @pl.loop(begin, end)
        def _(index):
            place = pl.ds(pl.multiple_of(index * step_e, step_e), step_e)
            edges_out[place, :] = (
                ecot[place, :].astype(F32) + dot_nt(edge_grad[place, :], ein[own_w, :])
            ).astype(BF16)

    blocks = edge_count // step_e
    edge_tail(0, blocks // 2)
    ein_c[1].planes()
    eout_c.place()
    edge_tail(blocks // 2, blocks)
    ein_c[0].finish()

    for step in range(1, domains):
        back_copies[step - 1].wait_recv()

    list_row = jnp.concatenate(
        [
            jnp.transpose(list_col[block : block + LANES, :])[0:1, :]
            for block in range(0, halo, LANES)
        ],
        axis=1,
    )
    back = returned[...].reshape(halo, width)

    def node_tail(begin, end):
        @pl.loop(begin, end)
        def _(index):
            start = pl.multiple_of(index * step_v, step_v)
            place = pl.ds(start, step_v)
            nodes_out[place, :] = (
                ncot[place, :].astype(F32)
                + dot_nt(node_grad[place, :], nin[near, :])
                + dot_nt(sums_from[place, :], ein[from_w, :])
                + dot_nt(sums_to[place, :], ein[to_w, :])
                + dot(pick_columns(list_row, start, step_v), back)
            ).astype(BF16)

    blocks = node_count // step_v
    node_tail(0, blocks // 2)
    ein_c[1].layers()
    ein_c[0].place()
    node_tail(blocks // 2, blocks)
    ein_c[1].finish()
    ein_c[1].place()
    for copy in sent:
        copy.wait_send()


def layer(args, domains, planes, layers):
    nodes, edges, ncot, ecot, senders, receivers, lists, ein, eout, egain, nin, nout, ngain = args
    node_count, width = nodes.shape
    edge_count = edges.shape[0]
    slots = lists.shape[0]
    halo = domains * slots
    half = width // 2
    plan = (
        ("nout", 0, half),
        ("nin", 0, half),
        ("eout", 0, half),
        ("ein", 0, half // 2),
        ("ein", half, half // 2),
    )
    rows = {"ein": 3 * width, "eout": width, "nin": 2 * width, "nout": width}
    dma = pltpu.SemaphoreType.DMA
    vmem = pltpu.VMEM
    anywhere = pl.BlockSpec(memory_space=pl.ANY)
    inside = pl.BlockSpec(memory_space=pltpu.VMEM)
    share = {name: count // domains for name, count in rows.items()}
    out_shape = (
        jax.ShapeDtypeStruct((edge_count, width), BF16),
        jax.ShapeDtypeStruct((node_count, width), BF16),
        jax.ShapeDtypeStruct((share["ein"], width), F32),
        jax.ShapeDtypeStruct((share["eout"], width), F32),
        jax.ShapeDtypeStruct((share["nin"], width), F32),
        jax.ShapeDtypeStruct((share["nout"], width), F32),
        jax.ShapeDtypeStruct((8, width), F32),
    )
    scratch = [vmem(arg.shape, arg.dtype) for arg in args]
    scratch += [
        vmem((edge_count, LANES), I32),
        vmem((edge_count, LANES), I32),
        vmem((halo, LANES), I32),
        vmem((domains, slots, width), BF16),
        vmem((domains, slots, width), BF16),
        vmem((node_count, width), BF16),
        vmem((node_count, width), BF16),
        vmem((halo, width), BF16),
        vmem((edge_count, width), F32),
        vmem((edge_count, width), F32),
        vmem((edge_count, width), BF16),
        vmem((edge_count, width), F32),
        vmem((edge_count, LANES), F32),
        vmem((edge_count, width), BF16),
        vmem((edge_count, width), BF16),
        vmem((node_count, width), BF16),
        vmem((node_count, width), BF16),
        vmem((node_count, width), BF16),
        vmem((node_count, width), BF16),
        vmem((node_count, width), BF16),
        vmem((node_count + halo, width), BF16),
        vmem((node_count, width), BF16),
        vmem((domains, slots, width), BF16),
        vmem((domains, slots, width), BF16),
        vmem((3 * width, width), BF16),
        vmem((width, width), BF16),
        vmem((2 * width, width), BF16),
        vmem((width, width), BF16),
        vmem((16, width), F32),
        vmem((8, width), F32),
        vmem((8, width), F32),
        vmem((planes - 1, 8, width), F32),
        vmem((8, width), F32),
        vmem((layers - 1, 8, width), F32),
        dma((13,)),
        dma((2, domains - 1)),
        dma((2, domains - 1)),
        dma((2, planes + layers - 1)),
    ]
    for name, _, wide in plan:
        count = share[name]
        scratch += [
            vmem((rows[name], wide), BF16),
            vmem((layers, planes, count, wide), BF16),
            vmem((planes - 1, layers, count, wide), BF16),
            vmem((layers, count, wide), BF16),
            vmem((layers - 1, count, wide), BF16),
            vmem((count, wide), BF16),
            vmem((count, wide), BF16),
            dma((2, planes + layers)),
        ]
    shape = (node_count, edge_count, width, domains, slots, planes, layers, plan)
    return pl.pallas_call(
        functools.partial(layer_kernel, shape),
        out_shape=out_shape,
        in_specs=[anywhere] * len(args),
        out_specs=(inside,) * len(out_shape),
        scratch_shapes=scratch,
        compiler_params=pltpu.CompilerParams(
            collective_id=0, has_side_effects=True, vmem_limit_bytes=63 * 1024 * 1024
        ),
        name="layer",
    )(*args)


def local(
    nodes, edges, node_cotangent, edge_cotangent, senders, receivers, send_rows,
    edge_in, edge_out, edge_gain, node_in, node_out, node_gain,
):
    domains = lax.axis_size("dom")
    planes = 1
    while planes * planes < domains:
        planes *= 2
    width = nodes.shape[2]
    args = (
        nodes[0], edges[0], node_cotangent[0], edge_cotangent[0], senders, receivers,
        send_rows[0].T, edge_in, edge_out, edge_gain[None], node_in, node_out, node_gain[None],
    )
    results = layer(args, domains, planes, domains // planes)
    grad_edges, grad_nodes, ein, eout, nin, nout, gains = results
    share = width // domains
    own = lax.dynamic_slice_in_dim(gains, lax.axis_index("dom") * share, share, 1)
    return grad_edges[None], grad_nodes[None], ein, eout, nin, nout, own[0], own[1]


def solution(mesh):
    placed = (
        P("group", "dom", None),
        P("group", "dom", None),
        P("group", "dom", None),
        P("group", "dom", None),
        P("group", "dom"),
        P("group", "dom"),
        P("group", "dom", None),
        P(),
        P(),
        P(),
        P(),
        P(),
        P(),
    )
    return jax.shard_map(
        local,
        mesh=mesh,
        in_specs=placed,
        out_specs=(
            P("group", "dom", None),
            P("group", "dom", None),
            P("dom", None),
            P("dom", None),
            P("dom", None),
            P("dom", None),
            P("dom"),
            P("dom"),
        ),
        check_vma=False,
    )
```

```python
import functools

import jax
import jax.numpy as jnp
from jax import lax
from jax.experimental import pallas as pl
from jax.experimental.pallas import tpu as pltpu
from jax.sharding import PartitionSpec as P

MESH = pl.DeviceIdType.MESH
F32 = jnp.float32
BF16 = jnp.bfloat16
I32 = jnp.int32
LANES = 128


def dot(first, second):
    return jnp.dot(first, second, preferred_element_type=F32)


def dot_tn(first, second):
    return lax.dot_general(first, second, (((0,), (0,)), ((), ())), preferred_element_type=F32)


def dot_nt(first, second):
    return lax.dot_general(first, second, (((1,), (1,)), ((), ())), preferred_element_type=F32)


def normalize(hidden):
    centre = hidden - jnp.mean(hidden, axis=-1, keepdims=True)
    inverse = lax.rsqrt(jnp.mean(centre * centre, axis=-1, keepdims=True) + 1e-05)
    return centre * inverse, inverse


def norm_back(upstream, gain, normed, inverse):
    scaled = upstream * gain
    return inverse * (
        scaled
        - jnp.mean(scaled, axis=-1, keepdims=True)
        - normed * jnp.mean(scaled * normed, axis=-1, keepdims=True)
    )


def swish_pair(value):
    logistic = jax.nn.sigmoid(value)
    return value * logistic, logistic * (1.0 + value * (1.0 - logistic))


def hot(mask):
    return jnp.where(mask, 1.0, 0.0).astype(BF16)


def pick_rows(column, base, count):
    lane = lax.broadcasted_iota(I32, column.shape, 1)
    return jnp.concatenate(
        [hot(column == lane + (base + block)) for block in range(0, count, LANES)], axis=1
    )


def pick_columns(row, base, count):
    index = lax.broadcasted_iota(I32, (count, row.shape[1]), 0) + base
    return hot(index == row)


def fold(value):
    return jnp.sum(value.reshape(value.shape[0] // 8, 8, value.shape[1]), axis=0)


def tile_of(count, sizes):
    return next(size for size in sizes if count % size == 0)


class Chunk:
    def __init__(self, env, mat, out, start, wide, refs):
        self.env, self.mat, self.out, self.start, self.wide = env, mat, out, start, wide
        (
            self.from_graph, self.sum_graph, self.from_first, self.sum_first, self.from_second,
            self.sum_second, self.from_layer, self.total, self.from_other, self.sem,
        ) = refs
        self.slot = 0

    def send(self, src, dst, device):
        slot = self.slot
        self.slot += 1
        return self.env.send(src, dst, self.sem.at[0, slot], self.sem.at[1, slot], device)

    def columns(self, group):
        return pl.ds(pl.multiple_of(self.start + group * self.wide, LANES), self.wide)

    def graph(self):
        env = self.env
        self.graph_copy = self.send(
            self.mat.at[:, self.columns(env.other)], self.from_graph, (env.other, env.dom)
        )

    def first(self):
        env = self.env
        side = env.side
        count = self.total.shape[0]
        self.graph_copy.wait_recv()
        for index in range(env.layers * side * side):
            x, y, layer = index % side, index // side % side, index // (side * side)
            rows = slice(index * count, (index + 1) * count)
            value = self.mat[rows, self.columns(env.group)].astype(F32)
            value = value + self.from_graph[rows, :].astype(F32)
            self.sum_graph[x + env.group * (y - x), y + env.group * (x - y), layer] = value.astype(BF16)
        self.copies = []
        for step in range(1, side):
            target = lax.rem(env.head + step, side)
            self.copies.append(
                self.send(
                    self.sum_graph.at[target],
                    self.from_first.at[step - 1],
                    (env.group, env.base + target * env.head_stride + env.tail * env.tail_stride),
                )
            )

    def second(self):
        env = self.env
        value = self.sum_graph[env.head].astype(F32)
        for step in range(1, env.side):
            self.copies[step - 1].wait_recv()
            value = value + self.from_first[step - 1].astype(F32)
        self.sum_first[...] = value.astype(BF16)
        self.copies = []
        for step in range(1, env.side):
            target = lax.rem(env.tail + step, env.side)
            self.copies.append(
                self.send(
                    self.sum_first.at[target],
                    self.from_second.at[step - 1],
                    (env.group, env.base + env.head * env.head_stride + target * env.tail_stride),
                )
            )

    def along(self):
        env = self.env
        value = self.sum_first[env.tail].astype(F32)
        for step in range(1, env.side):
            self.copies[step - 1].wait_recv()
            value = value + self.from_second[step - 1].astype(F32)
        self.sum_second[...] = value.astype(BF16)
        self.copies = []
        for step in range(1, env.layers):
            target = lax.rem(env.layer + step, env.layers)
            self.copies.append(
                self.send(
                    self.sum_second.at[target],
                    self.from_layer.at[step - 1],
                    (env.group, target * env.planes + env.plane),
                )
            )

    def finish(self):
        env = self.env
        value = self.sum_second[env.layer].astype(F32)
        for step in range(1, env.layers):
            self.copies[step - 1].wait_recv()
            value = value + self.from_layer[step - 1].astype(F32)
        short = value.astype(BF16)
        self.total[...] = short
        self.other_copy = self.send(self.total, self.from_other, (env.other, env.dom))
        self.out[:, self.columns(env.group)] = short.astype(F32)

    def place(self):
        self.other_copy.wait_recv()
        self.out[:, self.columns(self.env.other)] = self.from_other[...].astype(F32)


class Env:
    pass


def layer_kernel(shape, *refs):
    node_count, edge_count, width, domains, slots, side, layers, plan = shape
    planes = side * side
    halo = domains * slots
    rows_all = node_count + halo
    inputs, refs = refs[:13], refs[13:]
    (edges_out, nodes_out, ein_out, eout_out, nin_out, nout_out, gain_out), refs = refs[:7], refs[7:]
    loaded, refs = refs[:13], refs[13:]
    (
        nodes, edges, ncot, ecot, send_row, recv_row, list_in, ein, eout, egain, nin, nout, ngain,
    ) = loaded
    (
        send_col, recv_col, list_col, outgoing, arrived, from_table, to_table, halo_table,
        even, odd, edge_slope, edge_act, edge_hat, edge_inv, edge_mid, edge_grad,
        gathered, node_act, node_mid, node_grad, gathered_grad, sums_from, sums_to, returning, returned,
        ein_grad, eout_grad, nin_grad, nout_grad,
        gains, gain_graph, gain_mine, gain_plane, gain_mid, gain_layer,
        load_sem, halo_sem, back_sem, gain_sem,
    ), refs = refs[:39], refs[39:]

    env = Env()
    env.group = lax.axis_index("group")
    env.dom = lax.axis_index("dom")
    env.other = 1 - env.group
    env.planes, env.layers, env.side = planes, layers, side
    env.layer = env.dom // planes
    env.plane = lax.rem(env.dom, planes)
    env.base = env.layer * planes
    x, y = lax.rem(env.plane, side), env.plane // side
    env.head, env.tail = x + env.group * (y - x), y + env.group * (x - y)
    env.head_stride = 1 + env.group * (side - 1)
    env.tail_stride = side - env.group * (side - 1)
    sent = []

    def send(src, dst, send_sem, recv_sem, device):
        copy = pltpu.make_async_remote_copy(
            src_ref=src, dst_ref=dst, send_sem=send_sem, recv_sem=recv_sem,
            device_id=device, device_id_type=MESH,
        )
        copy.start()
        sent.append(copy)
        return copy

    env.send = send

    def peer(step):
        return lax.rem(env.dom + step, domains)

    loads = [
        pltpu.make_async_copy(src, dst, load_sem.at[index])
        for index, (src, dst) in enumerate(zip(inputs, loaded))
    ]
    NODES, EDGES, NCOT, ECOT, SEND, RECV, LIST, EIN, EOUT, EGAIN, NIN, NOUT, NGAIN = range(13)
    for index in (LIST, NODES, SEND, RECV, EIN, EDGES, EOUT, EGAIN, NIN, NOUT, NGAIN, NCOT, ECOT):
        loads[index].start()

    barrier = pltpu.get_barrier_semaphore()
    pl.semaphore_signal(barrier, inc=1, device_id=(env.other, env.dom), device_id_type=MESH)
    for step in range(1, domains):
        pl.semaphore_signal(barrier, inc=1, device_id=(env.group, peer(step)), device_id_type=MESH)

    loads[LIST].wait()
    for index in range(domains):
        list_col[index * slots : (index + 1) * slots, :] = jnp.broadcast_to(
            list_in[:, index : index + 1], (slots, LANES)
        )
    loads[NODES].wait()
    outgoing[...] = (
        dot(pick_rows(list_col[...], 0, node_count), nodes[...])
        .astype(BF16)
        .reshape(domains, slots, width)
    )
    pl.semaphore_wait(barrier, domains)
    halo_copies = [
        send(
            outgoing.at[peer(step)],
            arrived.at[env.dom],
            halo_sem.at[0, step - 1],
            halo_sem.at[1, step - 1],
            (env.group, peer(step)),
        )
        for step in range(1, domains)
    ]
    arrived[env.dom] = outgoing[env.dom]

    loads[SEND].wait()
    loads[RECV].wait()

    for block in range(0, edge_count, LANES):
        place = slice(block, block + LANES)
        send_col[place, :] = jnp.transpose(jnp.broadcast_to(send_row[:, place], (LANES, LANES)))
        recv_col[place, :] = jnp.transpose(jnp.broadcast_to(recv_row[:, place], (LANES, LANES)))

    loads[EIN].wait()
    own_w = slice(0, width)
    from_w = slice(width, 2 * width)
    to_w = slice(2 * width, 3 * width)
    step_n = tile_of(node_count, (512, 256, 128))

    @pl.loop(0, node_count // step_n)
    def _(index):
        place = pl.ds(pl.multiple_of(index * step_n, step_n), step_n)
        from_table[place, :] = dot(nodes[place, :], ein[from_w, :]).astype(BF16)
        to_table[place, :] = dot(nodes[place, :], ein[to_w, :]).astype(BF16)

    for index in (EDGES, EOUT, EGAIN):
        loads[index].wait()
    step_e = tile_of(edge_count, (256, 128))

    def tile(index):
        return pl.ds(pl.multiple_of(index * step_e, step_e), step_e)

    def pipeline(begin, end, lead, follow, between=None):
        lead(begin, even)
        if between is not None:
            between()

        @pl.loop(0, (end - begin) // 2 - 1)
        def _(pair):
            index = begin + 2 * pair
            lead(index + 1, odd)
            follow(index, even)
            lead(index + 2, even)
            follow(index + 1, odd)

        lead(end - 1, odd)
        follow(end - 2, even)
        follow(end - 1, odd)

    def edge_lead(index, buffer):
        place = tile(index)
        buffer[...] = (
            dot(edges[place, :], ein[own_w, :])
            + dot(pick_rows(send_col[place, :], 0, node_count), from_table[...])
            + dot(pick_rows(recv_col[place, :], 0, node_count), to_table[...])
        )

    def halo_ready():
        for copy in halo_copies:
            copy.wait_recv()
        halo_table[...] = dot(arrived[...].reshape(halo, width), ein[from_w, :]).astype(BF16)

    def edge_follow(index, buffer):
        place = tile(index)
        value = buffer[...] + dot(
            pick_rows(send_col[place, :], node_count, halo), halo_table[...]
        )
        act, slope = swish_pair(value)
        act = act.astype(BF16)
        edge_act[place, :] = act
        edge_slope[place, :] = slope
        normed, inverse = normalize(dot(act, eout[...]))
        edge_hat[place, :] = normed
        edge_inv[place, :] = jnp.broadcast_to(inverse, (step_e, LANES))
        edge_mid[place, :] = (normed * egain[...]).astype(BF16)

    pipeline(0, edge_count // step_e, edge_lead, edge_follow, halo_ready)

    for index in (NIN, NOUT, NGAIN, NCOT):
        loads[index].wait()
    near = slice(0, width)
    far = slice(width, 2 * width)
    gains[...] = jnp.zeros_like(gains)
    step_v = tile_of(node_count, (256, 128))

    def collect(start):
        gathered[start : start + step_v, :] = dot(
            pick_columns(recv_row[...], start, step_v), edge_mid[...]
        ).astype(BF16)

    collect(0)
    for start in range(0, node_count, step_v):
        place = slice(start, start + step_v)
        if start + step_v < node_count:
            collect(start + step_v)
        act, slope = swish_pair(
            dot(nodes[place, :], nin[near, :]) + dot(gathered[place, :], nin[far, :])
        )
        act = act.astype(BF16)
        node_act[place, :] = act
        normed, inverse = normalize(dot(act, nout[...]))
        upstream = ncot[place, :].astype(F32)
        gains[8:16, :] += fold(upstream * normed)
        post = norm_back(upstream, ngain[...], normed, inverse).astype(BF16)
        node_mid[place, :] = post
        grad = (dot_nt(post, nout[...]) * slope).astype(BF16)
        node_grad[place, :] = grad
        gathered_grad[place, :] = dot_nt(grad, nin[far, :]).astype(BF16)

    chunks = {}
    mats = {"ein": ein_grad, "eout": eout_grad, "nin": nin_grad, "nout": nout_grad}
    outs = {"ein": ein_out, "eout": eout_out, "nin": nin_out, "nout": nout_out}
    for index, (name, start, wide) in enumerate(plan):
        chunks[name, start] = Chunk(
            env, mats[name], outs[name], start, wide, refs[index * 10 : (index + 1) * 10]
        )
    half = width // 2
    nout_c, nin_c, eout_c = chunks["nout", 0], chunks["nin", 0], chunks["eout", 0]
    ein_c = (chunks["ein", 0], chunks["ein", half])

    nout_grad[...] = dot_tn(node_act[...], node_mid[...]).astype(BF16)
    nout_c.graph()
    nin_grad[near, :] = dot_tn(nodes[...], node_grad[...]).astype(BF16)
    nin_grad[far, :] = dot_tn(gathered[...], node_grad[...]).astype(BF16)
    nin_c.graph()

    loads[ECOT].wait()

    def back_lead(index, buffer):
        place = tile(index)
        buffer[...] = dot(pick_rows(recv_col[place, :], 0, node_count), gathered_grad[...])

    def back_follow(index, buffer):
        place = tile(index)
        upstream = ecot[place, :].astype(F32) + buffer[...]
        normed = edge_hat[place, :]
        gains[0:8, :] += fold(upstream * normed)
        post = norm_back(upstream, egain[...], normed, edge_inv[place, 0:1]).astype(BF16)
        edge_mid[place, :] = post
        edge_grad[place, :] = (dot_nt(post, eout[...]) * edge_slope[place, :]).astype(BF16)

    blocks = edge_count // step_e
    pipeline(0, blocks // 2, back_lead, back_follow)
    nout_c.first()
    nin_c.first()
    pipeline(blocks // 2, blocks, back_lead, back_follow)

    gains[0:1, :] = jnp.sum(gains[0:8, :], axis=0, keepdims=True)
    gains[1:2, :] = jnp.sum(gains[8:16, :], axis=0, keepdims=True)
    gain_graph_copy = send(
        gains.at[0:8], gain_graph, gain_sem.at[0, 0], gain_sem.at[1, 0], (env.other, env.dom)
    )

    eout_grad[...] = dot_tn(edge_act[...], edge_mid[...]).astype(BF16)
    eout_c.graph()

    gain_graph_copy.wait_recv()
    gain_mine[...] = gains[0:8, :] + gain_graph[...]
    gain_copies = [
        send(
            gain_mine, gain_plane.at[step - 1], gain_sem.at[0, step], gain_sem.at[1, step],
            (env.group, env.base + lax.rem(env.plane + step, planes)),
        )
        for step in range(1, planes)
    ]

    step_s = tile_of(rows_all, (384, 256, 128))
    step_t = tile_of(node_count, (256, 128))

    def scatter_from(columns):
        @pl.loop(0, rows_all // step_s)
        def _(index):
            start = pl.multiple_of(index * step_s, LANES)
            sums_from[pl.ds(start, step_s), columns] = dot(
                pick_columns(send_row[...], start, step_s), edge_grad[:, columns]
            ).astype(BF16)

    def scatter_to(columns):
        @pl.loop(0, node_count // step_t)
        def _(index):
            start = pl.multiple_of(index * step_t, step_t)
            sums_to[pl.ds(start, step_t), columns] = dot(
                pick_columns(recv_row[...], start, step_t), edge_grad[:, columns]
            ).astype(BF16)

    def edge_in_grads(columns):
        ein_grad[own_w, columns] = dot_tn(edges[...], edge_grad[:, columns]).astype(BF16)
        ein_grad[from_w, columns] = (
            dot_tn(nodes[...], sums_from[0:node_count, columns])
            + dot_tn(arrived[...].reshape(halo, width), sums_from[node_count:rows_all, columns])
        ).astype(BF16)
        ein_grad[to_w, columns] = dot_tn(nodes[...], sums_to[:, columns]).astype(BF16)

    first, second = slice(0, half), slice(half, width)
    scatter_from(first)
    nout_c.second()
    eout_c.first()
    scatter_to(first)
    edge_in_grads(first)
    ein_c[0].graph()

    total = gain_mine[...]
    for step in range(1, planes):
        gain_copies[step - 1].wait_recv()
        total = total + gain_plane[step - 1]
    gain_mid[...] = total
    gain_copies = [
        send(
            gain_mid, gain_layer.at[step - 1],
            gain_sem.at[0, planes + step - 1], gain_sem.at[1, planes + step - 1],
            (env.group, lax.rem(env.layer + step, layers) * planes + env.plane),
        )
        for step in range(1, layers)
    ]
    nin_c.second()

    scatter_from(second)
    returning[...] = (
        dot_nt(sums_from[node_count:rows_all, :], ein[from_w, :])
        .astype(BF16)
        .reshape(domains, slots, width)
    )
    back_copies = [
        send(
            returning.at[peer(step)],
            returned.at[env.dom],
            back_sem.at[0, step - 1],
            back_sem.at[1, step - 1],
            (env.group, peer(step)),
        )
        for step in range(1, domains)
    ]
    returned[env.dom] = returning[env.dom]
    nout_c.along()
    ein_c[0].first()
    eout_c.second()
    scatter_to(second)
    edge_in_grads(second)
    ein_c[1].graph()
    nin_c.along()
    nout_c.finish()
    ein_c[0].second()
    eout_c.along()

    total = gain_mid[...]
    for step in range(1, layers):
        gain_copies[step - 1].wait_recv()
        total = total + gain_layer[step - 1]
    share = width // domains
    gain_out[...] = pltpu.roll(total, lax.rem(width - env.dom * share, width), 1)

    def edge_tail(begin, end):
        @pl.loop(begin, end)
        def _(index):
            place = pl.ds(pl.multiple_of(index * step_e, step_e), step_e)
            edges_out[place, :] = (
                ecot[place, :].astype(F32) + dot_nt(edge_grad[place, :], ein[own_w, :])
            ).astype(BF16)

    edge_tail(0, blocks // 2)
    ein_c[1].first()
    nout_c.place()
    edge_tail(blocks // 2, blocks)
    ein_c[0].along()
    nin_c.finish()

    for step in range(1, domains):
        back_copies[step - 1].wait_recv()

    list_row = jnp.concatenate(
        [
            jnp.transpose(list_col[block : block + LANES, :])[0:1, :]
            for block in range(0, halo, LANES)
        ],
        axis=1,
    )
    back = returned[...].reshape(halo, width)

    def node_tail(begin, end):
        @pl.loop(begin, end)
        def _(index):
            start = pl.multiple_of(index * step_v, step_v)
            place = pl.ds(start, step_v)
            nodes_out[place, :] = (
                ncot[place, :].astype(F32)
                + dot_nt(node_grad[place, :], nin[near, :])
                + dot_nt(sums_from[place, :], ein[from_w, :])
                + dot_nt(sums_to[place, :], ein[to_w, :])
                + dot(pick_columns(list_row, start, step_v), back)
            ).astype(BF16)

    blocks = node_count // step_v
    node_tail(0, blocks // 2)
    ein_c[1].second()
    eout_c.finish()
    nin_c.place()
    node_tail(blocks // 2, blocks)
    ein_c[0].finish()
    ein_c[1].along()
    eout_c.place()
    ein_c[0].place()
    ein_c[1].finish()
    ein_c[1].place()
    for copy in sent:
        copy.wait_send()


def layer(args, domains, side, layers):
    planes = side * side
    nodes, edges, ncot, ecot, senders, receivers, lists, ein, eout, egain, nin, nout, ngain = args
    node_count, width = nodes.shape
    edge_count = edges.shape[0]
    slots = lists.shape[0]
    halo = domains * slots
    half = width // 2
    plan = (
        ("nout", 0, half),
        ("nin", 0, half),
        ("eout", 0, half),
        ("ein", 0, half // 2),
        ("ein", half, half // 2),
    )
    rows = {"ein": 3 * width, "eout": width, "nin": 2 * width, "nout": width}
    dma = pltpu.SemaphoreType.DMA
    vmem = pltpu.VMEM
    anywhere = pl.BlockSpec(memory_space=pl.ANY)
    inside = pl.BlockSpec(memory_space=pltpu.VMEM)
    share = {name: count // domains for name, count in rows.items()}
    out_shape = (
        vmem((edge_count, width), BF16),
        vmem((node_count, width), BF16),
        vmem((share["ein"], width), F32),
        vmem((share["eout"], width), F32),
        vmem((share["nin"], width), F32),
        vmem((share["nout"], width), F32),
        vmem((8, width), F32),
    )
    scratch = [vmem(arg.shape, arg.dtype) for arg in args]
    scratch += [
        vmem((edge_count, LANES), I32),
        vmem((edge_count, LANES), I32),
        vmem((halo, LANES), I32),
        vmem((domains, slots, width), BF16),
        vmem((domains, slots, width), BF16),
        vmem((node_count, width), BF16),
        vmem((node_count, width), BF16),
        vmem((halo, width), BF16),
        vmem((256, width), F32),
        vmem((256, width), F32),
        vmem((edge_count, width), F32),
        vmem((edge_count, width), BF16),
        vmem((edge_count, width), F32),
        vmem((edge_count, LANES), F32),
        vmem((edge_count, width), BF16),
        vmem((edge_count, width), BF16),
        vmem((node_count, width), BF16),
        vmem((node_count, width), BF16),
        vmem((node_count, width), BF16),
        vmem((node_count, width), BF16),
        vmem((node_count, width), BF16),
        vmem((node_count + halo, width), BF16),
        vmem((node_count, width), BF16),
        vmem((domains, slots, width), BF16),
        vmem((domains, slots, width), BF16),
        vmem((3 * width, width), BF16),
        vmem((width, width), BF16),
        vmem((2 * width, width), BF16),
        vmem((width, width), BF16),
        vmem((16, width), F32),
        vmem((8, width), F32),
        vmem((8, width), F32),
        vmem((planes - 1, 8, width), F32),
        vmem((8, width), F32),
        vmem((layers - 1, 8, width), F32),
        dma((13,)),
        dma((2, domains - 1)),
        dma((2, domains - 1)),
        dma((2, planes + layers - 1)),
    ]
    for name, _, wide in plan:
        count = share[name]
        scratch += [
            vmem((rows[name], wide), BF16),
            vmem((side, side, layers, count, wide), BF16),
            vmem((side - 1, side, layers, count, wide), BF16),
            vmem((side, layers, count, wide), BF16),
            vmem((side - 1, layers, count, wide), BF16),
            vmem((layers, count, wide), BF16),
            vmem((layers - 1, count, wide), BF16),
            vmem((count, wide), BF16),
            vmem((count, wide), BF16),
            dma((2, 2 * side + layers - 1)),
        ]
    shape = (node_count, edge_count, width, domains, slots, side, layers, plan)
    return pl.pallas_call(
        functools.partial(layer_kernel, shape),
        out_shape=out_shape,
        in_specs=[anywhere] * len(args),
        out_specs=(inside,) * len(out_shape),
        scratch_shapes=scratch,
        compiler_params=pltpu.CompilerParams(
            collective_id=0, has_side_effects=True, vmem_limit_bytes=56 * 1024 * 1024
        ),
        name="layer",
    )(*args)


def hand_kernel(*refs):
    sources, targets, sems = refs[:7], refs[7:15], refs[15]
    copies = [
        pltpu.make_async_copy(source, target, sems.at[index])
        for index, (source, target) in enumerate(zip(sources[:6], targets[:6]))
    ]
    for copy in copies:
        copy.start()
    gains = sources[6]
    share = targets[6].shape[1]
    targets[6][...] = gains[0:1, 0:share]
    targets[7][...] = gains[1:2, 0:share]
    for copy in copies:
        copy.wait()


def hand_out(results, share):
    inside = pl.BlockSpec(memory_space=pltpu.VMEM)
    anywhere = pl.BlockSpec(memory_space=pl.ANY)
    return pl.pallas_call(
        hand_kernel,
        out_shape=tuple(jax.ShapeDtypeStruct(value.shape, value.dtype) for value in results[:6])
        + (jax.ShapeDtypeStruct((1, share), F32),) * 2,
        in_specs=[inside] * 7,
        out_specs=(anywhere,) * 6 + (inside,) * 2,
        scratch_shapes=[pltpu.SemaphoreType.DMA((6,))],
        compiler_params=pltpu.CompilerParams(vmem_limit_bytes=6 * 1024 * 1024),
        name="hand_out",
    )(*results)


def local(
    nodes, edges, node_cotangent, edge_cotangent, senders, receivers, send_rows,
    edge_in, edge_out, edge_gain, node_in, node_out, node_gain,
):
    domains = lax.axis_size("dom")
    side = 1
    while 8 * side**3 <= domains:
        side *= 2
    width = nodes.shape[2]
    args = (
        nodes[0], edges[0], node_cotangent[0], edge_cotangent[0], senders, receivers,
        send_rows[0].T, edge_in, edge_out, edge_gain[None], node_in, node_out, node_gain[None],
    )
    results = layer(args, domains, side, domains // (side * side))
    results = hand_out(results, width // domains)
    grad_edges, grad_nodes, ein, eout, nin, nout, edge_share, node_share = results
    return grad_edges[None], grad_nodes[None], ein, eout, nin, nout, edge_share[0], node_share[0]


def solution(mesh):
    placed = (
        P("group", "dom", None),
        P("group", "dom", None),
        P("group", "dom", None),
        P("group", "dom", None),
        P("group", "dom"),
        P("group", "dom"),
        P("group", "dom", None),
        P(),
        P(),
        P(),
        P(),
        P(),
        P(),
    )
    return jax.shard_map(
        local,
        mesh=mesh,
        in_specs=placed,
        out_specs=(
            P("group", "dom", None),
            P("group", "dom", None),
            P("dom", None),
            P("dom", None),
            P("dom", None),
            P("dom", None),
            P("dom"),
            P("dom"),
        ),
        check_vma=False,
    )
```

```python
import functools

import jax
import jax.numpy as jnp
from jax import lax
from jax.experimental import pallas as pl
from jax.experimental.pallas import tpu as pltpu
from jax.sharding import PartitionSpec as P

MESH = pl.DeviceIdType.MESH
F32 = jnp.float32
BF16 = jnp.bfloat16
I32 = jnp.int32
LANES = 128


def dot(first, second):
    return jnp.dot(first, second, preferred_element_type=F32)


def dot_tn(first, second):
    return lax.dot_general(first, second, (((0,), (0,)), ((), ())), preferred_element_type=F32)


def dot_nt(first, second):
    return lax.dot_general(first, second, (((1,), (1,)), ((), ())), preferred_element_type=F32)


def normalize(hidden):
    centre = hidden - jnp.mean(hidden, axis=-1, keepdims=True)
    inverse = lax.rsqrt(jnp.mean(centre * centre, axis=-1, keepdims=True) + 1e-05)
    return centre * inverse, inverse


def norm_back(upstream, gain, normed, inverse):
    scaled = upstream * gain
    return inverse * (
        scaled
        - jnp.mean(scaled, axis=-1, keepdims=True)
        - normed * jnp.mean(scaled * normed, axis=-1, keepdims=True)
    )


def swish_pair(value):
    logistic = jax.nn.sigmoid(value)
    return value * logistic, logistic * (1.0 + value * (1.0 - logistic))


def hot(mask):
    return jnp.where(mask, 1.0, 0.0).astype(BF16)


def pick_rows(column, base, count):
    lane = lax.broadcasted_iota(I32, column.shape, 1)
    return jnp.concatenate(
        [hot(column == lane + (base + block)) for block in range(0, count, LANES)], axis=1
    )


def pick_columns(row, base, count):
    index = lax.broadcasted_iota(I32, (count, row.shape[1]), 0) + base
    return hot(index == row)


def fold(value):
    return jnp.sum(value.reshape(value.shape[0] // 8, 8, value.shape[1]), axis=0)


def tile_of(count, sizes):
    return next(size for size in sizes if count % size == 0)


class Chunk:
    def __init__(self, env, mat, out, start, wide, begin, end, refs):
        self.env, self.mat, self.out, self.start, self.wide = env, mat, out, start, wide
        self.begin, self.end = begin, end
        (
            self.from_graph, self.sum_graph, self.from_first, self.sum_first, self.from_second,
            self.sum_second, self.from_layer, self.total, self.from_other, self.sem,
        ) = refs
        self.slot = 0
        whole = begin == 0 and end == env.layers
        self.mine = None if whole else self.owned(env.layer)
        self.whole = whole
        first_row = begin * env.planes * self.total.shape[0]
        self.rows = slice(first_row, first_row + self.from_graph.shape[0])

    def owned(self, layer):
        return jnp.logical_and(layer >= self.begin, layer < self.end)

    def send(self, src, dst, device, when=None):
        slot = self.slot
        self.slot += 1
        return self.env.send(src, dst, self.sem.at[0, slot], self.sem.at[1, slot], device, when)

    def columns(self, group):
        return pl.ds(pl.multiple_of(self.start + group * self.wide, LANES), self.wide)

    def graph(self):
        env = self.env
        self.graph_copy = self.send(
            self.mat.at[self.rows, self.columns(env.other)], self.from_graph, (env.other, env.dom)
        )

    def first(self):
        env = self.env
        side = env.side
        count = self.total.shape[0]
        self.graph_copy.wait_recv()
        for index in range((self.end - self.begin) * side * side):
            x, y, layer = index % side, index // side % side, index // (side * side)
            rows = slice(index * count, (index + 1) * count)
            there = slice(self.rows.start + rows.start, self.rows.start + rows.stop)
            value = self.mat[there, self.columns(env.group)].astype(F32)
            value = value + self.from_graph[rows, :].astype(F32)
            self.sum_graph[x + env.group * (y - x), y + env.group * (x - y), layer] = value.astype(BF16)
        self.copies = []
        for step in range(1, side):
            target = lax.rem(env.head + step, side)
            self.copies.append(
                self.send(
                    self.sum_graph.at[target],
                    self.from_first.at[step - 1],
                    (env.group, env.base + target * env.head_stride + env.tail * env.tail_stride),
                )
            )

    def second(self):
        env = self.env
        value = self.sum_graph[env.head].astype(F32)
        for step in range(1, env.side):
            self.copies[step - 1].wait_recv()
            value = value + self.from_first[step - 1].astype(F32)
        self.sum_first[...] = value.astype(BF16)
        self.copies = []
        for step in range(1, env.side):
            target = lax.rem(env.tail + step, env.side)
            self.copies.append(
                self.send(
                    self.sum_first.at[target],
                    self.from_second.at[step - 1],
                    (env.group, env.base + env.head * env.head_stride + target * env.tail_stride),
                )
            )

    def along(self):
        env = self.env
        value = self.sum_first[env.tail].astype(F32)
        for step in range(1, env.side):
            self.copies[step - 1].wait_recv()
            value = value + self.from_second[step - 1].astype(F32)
        self.sum_second[...] = value.astype(BF16)
        self.copies = []
        for step in range(1, env.layers):
            target = lax.rem(env.layer + step, env.layers)
            place = target if self.whole else jnp.clip(target - self.begin, 0, self.end - self.begin - 1)
            self.copies.append(
                self.send(
                    self.sum_second.at[place],
                    self.from_layer.at[step - 1],
                    (env.group, target * env.planes + env.plane),
                    None if self.whole else self.owned(target),
                )
            )

    def finish(self):
        env = self.env

        def last():
            place = env.layer - self.begin
            if not self.whole:
                place = jnp.clip(place, 0, self.end - self.begin - 1)
            value = self.sum_second[place].astype(F32)
            for step in range(1, env.layers):
                self.copies[step - 1].wait_recv()
                value = value + self.from_layer[step - 1].astype(F32)
            short = value.astype(BF16)
            self.total[...] = short
            self.out[:, self.columns(env.group)] = short.astype(F32)

        if self.whole:
            last()
        else:
            pl.when(self.mine)(last)
        self.other_copy = self.send(self.total, self.from_other, (env.other, env.dom), self.mine)

    def place(self):
        def last():
            self.other_copy.wait_recv()
            self.out[:, self.columns(self.env.other)] = self.from_other[...].astype(F32)

        if self.whole:
            last()
        else:
            pl.when(self.mine)(last)


class Env:
    pass


def layer_kernel(shape, *refs):
    node_count, edge_count, width, domains, slots, side, layers, plan = shape
    planes = side * side
    halo = domains * slots
    rows_all = node_count + halo
    inputs, refs = refs[:13], refs[13:]
    (edges_out, nodes_out, ein_out, eout_out, nin_out, nout_out, gain_out), refs = refs[:7], refs[7:]
    loaded, refs = refs[:13], refs[13:]
    (
        nodes, edges, ncot, ecot, send_row, recv_row, list_in, ein, eout, egain, nin, nout, ngain,
    ) = loaded
    (
        send_col, recv_col, list_col, outgoing, arrived, from_table, to_table, halo_table,
        even, odd, node_near, edge_slope, edge_act, edge_hat, edge_inv, edge_mid, edge_grad,
        gathered, node_act, node_mid, node_grad, gathered_grad, sums_from, sums_to, returning, returned,
        ein_grad, eout_grad, nin_grad, nout_grad,
        gains, gain_graph, gain_mine, gain_plane, gain_mid, gain_layer,
        load_sem, halo_sem, back_sem, gain_sem,
    ), refs = refs[:40], refs[40:]

    env = Env()
    env.group = lax.axis_index("group")
    env.dom = lax.axis_index("dom")
    env.other = 1 - env.group
    env.planes, env.layers, env.side = planes, layers, side
    env.layer = env.dom // planes
    env.plane = lax.rem(env.dom, planes)
    env.base = env.layer * planes
    x, y = lax.rem(env.plane, side), env.plane // side
    env.head, env.tail = x + env.group * (y - x), y + env.group * (x - y)
    env.head_stride = 1 + env.group * (side - 1)
    env.tail_stride = side - env.group * (side - 1)
    sent = []

    def send(src, dst, send_sem, recv_sem, device, when=None):
        copy = pltpu.make_async_remote_copy(
            src_ref=src, dst_ref=dst, send_sem=send_sem, recv_sem=recv_sem,
            device_id=device, device_id_type=MESH,
        )
        if when is None:
            copy.start()
        else:
            pl.when(when)(copy.start)
        sent.append((copy, when))
        return copy

    env.send = send

    def drain():
        for copy, when in sent:
            if when is None:
                copy.wait_send()
            else:
                pl.when(when)(copy.wait_send)
        sent.clear()

    def peer(step):
        return lax.rem(env.dom + step, domains)

    loads = [
        pltpu.make_async_copy(src, dst, load_sem.at[index])
        for index, (src, dst) in enumerate(zip(inputs, loaded))
    ]
    NODES, EDGES, NCOT, ECOT, SEND, RECV, LIST, EIN, EOUT, EGAIN, NIN, NOUT, NGAIN = range(13)
    for index in (LIST, SEND, RECV, NODES, EIN, EDGES, EOUT, EGAIN, NIN, NOUT, NGAIN, NCOT, ECOT):
        loads[index].start()

    barrier = pltpu.get_barrier_semaphore()
    pl.semaphore_signal(barrier, inc=1, device_id=(env.other, env.dom), device_id_type=MESH)
    for step in range(1, domains):
        pl.semaphore_signal(barrier, inc=1, device_id=(env.group, peer(step)), device_id_type=MESH)

    loads[LIST].wait()
    for index in range(domains):
        list_col[index * slots : (index + 1) * slots, :] = jnp.broadcast_to(
            list_in[:, index : index + 1], (slots, LANES)
        )
    loads[SEND].wait()
    loads[RECV].wait()

    for block in range(0, edge_count, LANES):
        place = slice(block, block + LANES)
        send_col[place, :] = jnp.transpose(jnp.broadcast_to(send_row[:, place], (LANES, LANES)))
        recv_col[place, :] = jnp.transpose(jnp.broadcast_to(recv_row[:, place], (LANES, LANES)))

    loads[NODES].wait()
    outgoing[...] = (
        dot(pick_rows(list_col[...], 0, node_count), nodes[...])
        .astype(BF16)
        .reshape(domains, slots, width)
    )
    pl.semaphore_wait(barrier, domains)
    halo_copies = [
        send(
            outgoing.at[peer(step)],
            arrived.at[env.dom],
            halo_sem.at[0, step - 1],
            halo_sem.at[1, step - 1],
            (env.group, peer(step)),
        )
        for step in range(1, domains)
    ]
    arrived[env.dom] = outgoing[env.dom]

    loads[EIN].wait()
    own_w = slice(0, width)
    from_w = slice(width, 2 * width)
    to_w = slice(2 * width, 3 * width)
    step_n = tile_of(node_count, (512, 256, 128))

    @pl.loop(0, node_count // step_n)
    def _(index):
        place = pl.ds(pl.multiple_of(index * step_n, step_n), step_n)
        from_table[place, :] = dot(nodes[place, :], ein[from_w, :]).astype(BF16)
        to_table[place, :] = dot(nodes[place, :], ein[to_w, :]).astype(BF16)

    for index in (EDGES, EOUT, EGAIN):
        loads[index].wait()
    step_e = even.shape[0]
    blocks = edge_count // step_e

    def tile(index):
        return slice(index * step_e, (index + 1) * step_e)

    buffers = (even, odd)

    def edge_lead(index, buffer):
        place = tile(index)
        buffer[...] = (
            dot(edges[place, :], ein[own_w, :])
            + dot(pick_rows(send_col[place, :], 0, node_count), from_table[...])
            + dot(pick_rows(recv_col[place, :], 0, node_count), to_table[...])
        )

    def halo_ready():
        for copy in halo_copies:
            copy.wait_recv()
        halo_table[...] = dot(arrived[...].reshape(halo, width), ein[from_w, :]).astype(BF16)

    def edge_follow(index, buffer):
        place = tile(index)
        value = buffer[...] + dot(
            pick_rows(send_col[place, :], node_count, halo), halo_table[...]
        )
        act, slope = swish_pair(value)
        act = act.astype(BF16)
        edge_act[place, :] = act
        edge_slope[place, :] = slope
        normed, inverse = normalize(dot(act, eout[...]))
        edge_hat[place, :] = normed
        edge_inv[place, :] = jnp.broadcast_to(inverse, (step_e, LANES))
        edge_mid[place, :] = (normed * egain[...]).astype(BF16)

    edge_lead(0, buffers[0])
    edge_lead(1, buffers[1])
    loads[NIN].wait()
    near = slice(0, width)
    far = slice(width, 2 * width)
    node_near[...] = dot(nodes[...], nin[near, :])
    halo_ready()
    for index in range(blocks):
        edge_follow(index, buffers[index % 2])
        if index + 2 < blocks:
            edge_lead(index + 2, buffers[index % 2])

    for index in (NOUT, NGAIN, NCOT):
        loads[index].wait()
    gains[...] = jnp.zeros_like(gains)
    step_v = tile_of(node_count, (512, 256, 128))

    def collect(start):
        gathered[start : start + step_v, :] = dot(
            pick_columns(recv_row[...], start, step_v), edge_mid[...]
        ).astype(BF16)

    collect(0)
    for start in range(0, node_count, step_v):
        place = slice(start, start + step_v)
        if start + step_v < node_count:
            collect(start + step_v)
        act, slope = swish_pair(
            node_near[place, :] + dot(gathered[place, :], nin[far, :])
        )
        act = act.astype(BF16)
        node_act[place, :] = act
        normed, inverse = normalize(dot(act, nout[...]))
        upstream = ncot[place, :].astype(F32)
        gains[8:16, :] += fold(upstream * normed)
        post = norm_back(upstream, ngain[...], normed, inverse).astype(BF16)
        node_mid[place, :] = post
        grad = (dot_nt(post, nout[...]) * slope).astype(BF16)
        node_grad[place, :] = grad
        gathered_grad[place, :] = dot_nt(grad, nin[far, :]).astype(BF16)

    chunks = {}
    mats = {"ein": ein_grad, "eout": eout_grad, "nin": nin_grad, "nout": nout_grad}
    outs = {"ein": ein_out, "eout": eout_out, "nin": nin_out, "nout": nout_out}
    for index, (name, start, wide, begin, end) in enumerate(plan):
        chunks[name, start, begin] = Chunk(
            env, mats[name], outs[name], start, wide, begin, end, refs[index * 10 : (index + 1) * 10]
        )
    half = width // 2
    nout_c, nin_c, eout_c = (chunks[name, 0, 0] for name in ("nout", "nin", "eout"))
    low_c = (chunks["ein", 0, 0], chunks["ein", half, 0])
    high_c = (chunks["ein", 0, layers // 2], chunks["ein", half, layers // 2])

    nout_grad[...] = dot_tn(node_act[...], node_mid[...]).astype(BF16)
    nout_c.graph()
    nin_grad[near, :] = dot_tn(nodes[...], node_grad[...]).astype(BF16)
    nin_grad[far, :] = dot_tn(gathered[...], node_grad[...]).astype(BF16)
    nin_c.graph()

    loads[ECOT].wait()

    def back_lead(index, buffer):
        place = tile(index)
        buffer[...] = dot(pick_rows(recv_col[place, :], 0, node_count), gathered_grad[...])

    def back_follow(index, buffer):
        place = tile(index)
        upstream = ecot[place, :].astype(F32) + buffer[...]
        normed = edge_hat[place, :]
        gains[0:8, :] += fold(upstream * normed)
        post = norm_back(upstream, egain[...], normed, edge_inv[place, 0:1]).astype(BF16)
        edge_mid[place, :] = post
        edge_grad[place, :] = (dot_nt(post, eout[...]) * edge_slope[place, :]).astype(BF16)

    back_lead(0, buffers[0])
    for index in range(blocks):
        if index + 1 < blocks:
            back_lead(index + 1, buffers[(index + 1) % 2])
        back_follow(index, buffers[index % 2])
        if index == 0:
            nout_c.first()
            nin_c.first()

    gains[0:1, :] = jnp.sum(gains[0:8, :], axis=0, keepdims=True)
    gains[1:2, :] = jnp.sum(gains[8:16, :], axis=0, keepdims=True)
    gain_graph_copy = send(
        gains.at[0:8], gain_graph, gain_sem.at[0, 0], gain_sem.at[1, 0], (env.other, env.dom)
    )

    step_s = tile_of(rows_all, (576, 512, 384, 256, 128))
    step_t = tile_of(node_count, (512, 256, 128))

    def scatter_from(columns):
        @pl.loop(0, rows_all // step_s)
        def _(index):
            start = pl.multiple_of(index * step_s, 64)
            sums_from[pl.ds(start, step_s), columns] = dot(
                pick_columns(send_row[...], start, step_s), edge_grad[:, columns]
            ).astype(BF16)

    def scatter_to(columns):
        @pl.loop(0, node_count // step_t)
        def _(index):
            start = pl.multiple_of(index * step_t, step_t)
            sums_to[pl.ds(start, step_t), columns] = dot(
                pick_columns(recv_row[...], start, step_t), edge_grad[:, columns]
            ).astype(BF16)

    def own_and_from(columns):
        ein_grad[own_w, columns] = dot_tn(edges[...], edge_grad[:, columns]).astype(BF16)
        ein_grad[from_w, columns] = (
            dot_tn(nodes[...], sums_from[0:node_count, columns])
            + dot_tn(arrived[...].reshape(halo, width), sums_from[node_count:rows_all, columns])
        ).astype(BF16)

    def toward(columns):
        ein_grad[to_w, columns] = dot_tn(nodes[...], sums_to[:, columns]).astype(BF16)

    first, second = slice(0, half), slice(half, width)
    eout_grad[...] = dot_tn(edge_act[...], edge_mid[...]).astype(BF16)
    eout_c.graph()
    nout_c.second()

    scatter_from(first)
    eout_c.first()
    gain_graph_copy.wait_recv()
    gain_mine[...] = gains[0:8, :] + gain_graph[...]
    gain_copies = [
        send(
            gain_mine, gain_plane.at[step - 1], gain_sem.at[0, step], gain_sem.at[1, step],
            (env.group, env.base + lax.rem(env.plane + step, planes)),
        )
        for step in range(1, planes)
    ]
    own_and_from(first)
    low_c[0].graph()
    nin_c.second()
    scatter_to(first)
    low_c[0].first()
    nout_c.along()
    toward(first)
    high_c[0].graph()

    scatter_from(second)
    returning[...] = (
        dot_nt(sums_from[node_count:rows_all, :], ein[from_w, :])
        .astype(BF16)
        .reshape(domains, slots, width)
    )
    back_copies = [
        send(
            returning.at[peer(step)],
            returned.at[env.dom],
            back_sem.at[0, step - 1],
            back_sem.at[1, step - 1],
            (env.group, peer(step)),
        )
        for step in range(1, domains)
    ]
    returned[env.dom] = returning[env.dom]
    high_c[0].first()
    eout_c.second()
    total = gain_mine[...]
    for step in range(1, planes):
        gain_copies[step - 1].wait_recv()
        total = total + gain_plane[step - 1]
    gain_mid[...] = total
    gain_copies = [
        send(
            gain_mid, gain_layer.at[step - 1],
            gain_sem.at[0, planes + step - 1], gain_sem.at[1, planes + step - 1],
            (env.group, lax.rem(env.layer + step, layers) * planes + env.plane),
        )
        for step in range(1, layers)
    ]
    own_and_from(second)
    low_c[1].graph()
    nin_c.along()
    scatter_to(second)
    low_c[1].first()
    low_c[0].second()
    eout_c.along()
    toward(second)
    high_c[1].graph()

    def edge_tail(begin, end):
        for index in range(begin, end):
            place = tile(index)
            edges_out[place, :] = (
                ecot[place, :].astype(F32) + dot_nt(edge_grad[place, :], ein[own_w, :])
            ).astype(BF16)

    edge_tail(0, blocks)
    high_c[1].first()
    high_c[0].second()
    low_c[0].along()

    for step in range(1, domains):
        back_copies[step - 1].wait_recv()

    list_row = jnp.concatenate(
        [
            jnp.transpose(list_col[block : block + LANES, :])[0:1, :]
            for block in range(0, halo, LANES)
        ],
        axis=1,
    )
    back = returned[...].reshape(halo, width)

    def node_tail(begin, end):
        for start in range(begin * step_v, end * step_v, step_v):
            place = slice(start, start + step_v)
            nodes_out[place, :] = (
                ncot[place, :].astype(F32)
                + dot_nt(node_grad[place, :], nin[near, :])
                + dot_nt(sums_from[place, :], ein[from_w, :])
                + dot_nt(sums_to[place, :], ein[to_w, :])
                + dot(pick_columns(list_row, start, step_v), back)
            ).astype(BF16)

    blocks = node_count // step_v
    node_tail(0, blocks // 2)
    low_c[1].second()
    nout_c.finish()
    node_tail(blocks // 2, blocks)
    high_c[0].along()
    high_c[1].second()
    low_c[1].along()
    nin_c.finish()
    total = gain_mid[...]
    for step in range(1, layers):
        gain_copies[step - 1].wait_recv()
        total = total + gain_layer[step - 1]
    share = width // domains
    gain_out[...] = pltpu.roll(total, lax.rem(width - env.dom * share, width), 1)
    nout_c.place()
    eout_c.finish()
    high_c[1].along()
    low_c[0].finish()
    nin_c.place()
    high_c[0].finish()
    eout_c.place()
    low_c[1].finish()
    low_c[0].place()
    high_c[0].place()
    high_c[1].finish()
    low_c[1].place()
    high_c[1].place()
    drain()


def layer(args, domains, side, layers):
    planes = side * side
    nodes, edges, ncot, ecot, senders, receivers, lists, ein, eout, egain, nin, nout, ngain = args
    node_count, width = nodes.shape
    edge_count = edges.shape[0]
    slots = lists.shape[0]
    halo = domains * slots
    half = width // 2
    tile = tile_of(edge_count // 4, (512, 256, 128))
    plan = (
        ("nout", 0, half, 0, layers),
        ("nin", 0, half, 0, layers),
        ("eout", 0, half, 0, layers),
        ("ein", 0, half // 2, 0, layers // 2),
        ("ein", 0, half // 2, layers // 2, layers),
        ("ein", half, half // 2, 0, layers // 2),
        ("ein", half, half // 2, layers // 2, layers),
    )
    rows = {"ein": 3 * width, "eout": width, "nin": 2 * width, "nout": width}
    dma = pltpu.SemaphoreType.DMA
    vmem = pltpu.VMEM
    anywhere = pl.BlockSpec(memory_space=pl.ANY)
    inside = pl.BlockSpec(memory_space=pltpu.VMEM)
    share = {name: count // domains for name, count in rows.items()}
    out_shape = (
        vmem((edge_count, width), BF16),
        vmem((node_count, width), BF16),
        vmem((share["ein"], width), F32),
        vmem((share["eout"], width), F32),
        vmem((share["nin"], width), F32),
        vmem((share["nout"], width), F32),
        vmem((8, width), F32),
    )
    scratch = [vmem(arg.shape, arg.dtype) for arg in args]
    scratch += [
        vmem((edge_count, LANES), I32),
        vmem((edge_count, LANES), I32),
        vmem((halo, LANES), I32),
        vmem((domains, slots, width), BF16),
        vmem((domains, slots, width), BF16),
        vmem((node_count, width), BF16),
        vmem((node_count, width), BF16),
        vmem((halo, width), BF16),
        vmem((tile, width), F32),
        vmem((tile, width), F32),
        vmem((node_count, width), F32),
        vmem((edge_count, width), F32),
        vmem((edge_count, width), BF16),
        vmem((edge_count, width), F32),
        vmem((edge_count, LANES), F32),
        vmem((edge_count, width), BF16),
        vmem((edge_count, width), BF16),
        vmem((node_count, width), BF16),
        vmem((node_count, width), BF16),
        vmem((node_count, width), BF16),
        vmem((node_count, width), BF16),
        vmem((node_count, width), BF16),
        vmem((node_count + halo, width), BF16),
        vmem((node_count, width), BF16),
        vmem((domains, slots, width), BF16),
        vmem((domains, slots, width), BF16),
        vmem((3 * width, width), BF16),
        vmem((width, width), BF16),
        vmem((2 * width, width), BF16),
        vmem((width, width), BF16),
        vmem((16, width), F32),
        vmem((8, width), F32),
        vmem((8, width), F32),
        vmem((planes - 1, 8, width), F32),
        vmem((8, width), F32),
        vmem((layers - 1, 8, width), F32),
        dma((13,)),
        dma((2, domains - 1)),
        dma((2, domains - 1)),
        dma((2, planes + layers - 1)),
    ]
    for name, _, wide, begin, end in plan:
        count = share[name]
        some = end - begin
        scratch += [
            vmem((some * planes * count, wide), BF16),
            vmem((side, side, some, count, wide), BF16),
            vmem((side - 1, side, some, count, wide), BF16),
            vmem((side, some, count, wide), BF16),
            vmem((side - 1, some, count, wide), BF16),
            vmem((some, count, wide), BF16),
            vmem((layers - 1, count, wide), BF16),
            vmem((count, wide), BF16),
            vmem((count, wide), BF16),
            dma((2, 2 * side + layers - 1)),
        ]
    shape = (node_count, edge_count, width, domains, slots, side, layers, plan)
    return pl.pallas_call(
        functools.partial(layer_kernel, shape),
        out_shape=out_shape,
        in_specs=[anywhere] * len(args),
        out_specs=(inside,) * len(out_shape),
        scratch_shapes=scratch,
        compiler_params=pltpu.CompilerParams(
            collective_id=0, has_side_effects=True, vmem_limit_bytes=56 * 1024 * 1024
        ),
        name="layer",
    )(*args)


def hand_kernel(*refs):
    sources, targets, shares, sems = refs[:7], refs[7:15], refs[15:17], refs[17]
    share = shares[0].shape[1]
    for row in range(2):
        shares[row][...] = sources[6][row : row + 1, 0:share]
    copies = [
        pltpu.make_async_copy(source, target, sems.at[index])
        for index, (source, target) in enumerate(zip(sources[:6] + shares, targets))
    ]
    for copy in copies:
        copy.start()
    for copy in copies:
        copy.wait()


def hand_out(results, share):
    inside = pl.BlockSpec(memory_space=pltpu.VMEM)
    anywhere = pl.BlockSpec(memory_space=pl.ANY)
    return pl.pallas_call(
        hand_kernel,
        out_shape=tuple(jax.ShapeDtypeStruct(value.shape, value.dtype) for value in results[:6])
        + (jax.ShapeDtypeStruct((1, share), F32),) * 2,
        in_specs=[inside] * 7,
        out_specs=(anywhere,) * 8,
        scratch_shapes=[pltpu.VMEM((1, share), F32), pltpu.VMEM((1, share), F32), pltpu.SemaphoreType.DMA((8,))],
        compiler_params=pltpu.CompilerParams(vmem_limit_bytes=6 * 1024 * 1024),
        name="hand_out",
    )(*results)


def local(
    nodes, edges, node_cotangent, edge_cotangent, senders, receivers, send_rows,
    edge_in, edge_out, edge_gain, node_in, node_out, node_gain,
):
    domains = lax.axis_size("dom")
    side = 1
    while 8 * side**3 <= domains:
        side *= 2
    width = nodes.shape[2]
    args = (
        nodes[0], edges[0], node_cotangent[0], edge_cotangent[0], senders, receivers,
        send_rows[0].T, edge_in, edge_out, edge_gain[None], node_in, node_out, node_gain[None],
    )
    results = layer(args, domains, side, domains // (side * side))
    results = hand_out(results, width // domains)
    grad_edges, grad_nodes, ein, eout, nin, nout, edge_share, node_share = results
    return grad_edges[None], grad_nodes[None], ein, eout, nin, nout, edge_share[0], node_share[0]


def solution(mesh):
    placed = (
        P("group", "dom", None),
        P("group", "dom", None),
        P("group", "dom", None),
        P("group", "dom", None),
        P("group", "dom"),
        P("group", "dom"),
        P("group", "dom", None),
        P(),
        P(),
        P(),
        P(),
        P(),
        P(),
    )
    return jax.shard_map(
        local,
        mesh=mesh,
        in_specs=placed,
        out_specs=(
            P("group", "dom", None),
            P("group", "dom", None),
            P("dom", None),
            P("dom", None),
            P("dom", None),
            P("dom", None),
            P("dom"),
            P("dom"),
        ),
        check_vma=False,
    )
```

```python
import functools

import jax
import jax.numpy as jnp
from jax import lax
from jax.experimental import pallas as pl
from jax.experimental.pallas import tpu as pltpu
from jax.sharding import PartitionSpec as P

MESH = pl.DeviceIdType.MESH
F32 = jnp.float32
BF16 = jnp.bfloat16
I32 = jnp.int32
LANES = 128


def dot(first, second):
    return jnp.dot(first, second, preferred_element_type=F32)


def dot_tn(first, second):
    return lax.dot_general(first, second, (((0,), (0,)), ((), ())), preferred_element_type=F32)


def dot_nt(first, second):
    return lax.dot_general(first, second, (((1,), (1,)), ((), ())), preferred_element_type=F32)


def normalize(hidden):
    centre = hidden - jnp.mean(hidden, axis=-1, keepdims=True)
    inverse = lax.rsqrt(jnp.mean(centre * centre, axis=-1, keepdims=True) + 1e-05)
    return centre * inverse, inverse


def norm_back(upstream, gain, normed, inverse):
    scaled = upstream * gain
    return inverse * (
        scaled
        - jnp.mean(scaled, axis=-1, keepdims=True)
        - normed * jnp.mean(scaled * normed, axis=-1, keepdims=True)
    )


def swish_pair(value):
    logistic = jax.nn.sigmoid(value)
    return value * logistic, logistic * (1.0 + value * (1.0 - logistic))


def hot(mask):
    return jnp.where(mask, 1.0, 0.0).astype(BF16)


def pick_rows(column, base, count):
    lane = lax.broadcasted_iota(I32, column.shape, 1)
    return jnp.concatenate(
        [hot(column == lane + (base + block)) for block in range(0, count, LANES)], axis=1
    )


def pick_columns(row, base, count):
    index = lax.broadcasted_iota(I32, (count, row.shape[1]), 0) + base
    return hot(index == row)


def fold(value):
    return jnp.sum(value.reshape(value.shape[0] // 8, 8, value.shape[1]), axis=0)


def tile_of(count, sizes):
    return next(size for size in sizes if count % size == 0)


class Chunk:
    def __init__(self, env, mat, out, start, wide, begin, end, refs):
        self.env, self.mat, self.out, self.start, self.wide = env, mat, out, start, wide
        self.begin, self.end = begin, end
        (
            self.from_graph, self.sum_graph, self.from_first, self.sum_first, self.from_second,
            self.sum_second, self.from_layer, self.total, self.from_other, self.sem,
        ) = refs
        self.slot = 0
        whole = begin == 0 and end == env.layers
        self.mine = None if whole else self.owned(env.layer)
        self.whole = whole
        first_row = begin * env.planes * self.total.shape[0]
        self.rows = slice(first_row, first_row + self.from_graph.shape[0])

    def owned(self, layer):
        return jnp.logical_and(layer >= self.begin, layer < self.end)

    def send(self, src, dst, device, when=None):
        slot = self.slot
        self.slot += 1
        return self.env.send(src, dst, self.sem.at[0, slot], self.sem.at[1, slot], device, when)

    def columns(self, group):
        return pl.ds(pl.multiple_of(self.start + group * self.wide, LANES), self.wide)

    def graph(self):
        env = self.env
        self.graph_copy = self.send(
            self.mat.at[self.rows, self.columns(env.other)], self.from_graph, (env.other, env.dom)
        )

    def first(self):
        env = self.env
        side = env.side
        count = self.total.shape[0]
        self.graph_copy.wait_recv()
        for index in range((self.end - self.begin) * side * side):
            x, y, layer = index % side, index // side % side, index // (side * side)
            rows = slice(index * count, (index + 1) * count)
            there = slice(self.rows.start + rows.start, self.rows.start + rows.stop)
            value = self.mat[there, self.columns(env.group)].astype(F32)
            value = value + self.from_graph[rows, :].astype(F32)
            self.sum_graph[x + env.group * (y - x), y + env.group * (x - y), layer] = value.astype(BF16)
        self.copies = []
        for step in range(1, side):
            target = lax.rem(env.head + step, side)
            self.copies.append(
                self.send(
                    self.sum_graph.at[target],
                    self.from_first.at[step - 1],
                    (env.group, env.base + target * env.head_stride + env.tail * env.tail_stride),
                )
            )

    def second(self):
        env = self.env
        value = self.sum_graph[env.head].astype(F32)
        for step in range(1, env.side):
            self.copies[step - 1].wait_recv()
            value = value + self.from_first[step - 1].astype(F32)
        self.sum_first[...] = value.astype(BF16)
        self.copies = []
        for step in range(1, env.side):
            target = lax.rem(env.tail + step, env.side)
            self.copies.append(
                self.send(
                    self.sum_first.at[target],
                    self.from_second.at[step - 1],
                    (env.group, env.base + env.head * env.head_stride + target * env.tail_stride),
                )
            )

    def along(self):
        env = self.env
        value = self.sum_first[env.tail].astype(F32)
        for step in range(1, env.side):
            self.copies[step - 1].wait_recv()
            value = value + self.from_second[step - 1].astype(F32)
        self.sum_second[...] = value.astype(BF16)
        self.copies = []
        for step in range(1, env.layers):
            target = lax.rem(env.layer + step, env.layers)
            place = target if self.whole else jnp.clip(target - self.begin, 0, self.end - self.begin - 1)
            self.copies.append(
                self.send(
                    self.sum_second.at[place],
                    self.from_layer.at[step - 1],
                    (env.group, target * env.planes + env.plane),
                    None if self.whole else self.owned(target),
                )
            )

    def finish(self):
        env = self.env

        def last():
            place = env.layer - self.begin
            if not self.whole:
                place = jnp.clip(place, 0, self.end - self.begin - 1)
            value = self.sum_second[place].astype(F32)
            for step in range(1, env.layers):
                self.copies[step - 1].wait_recv()
                value = value + self.from_layer[step - 1].astype(F32)
            short = value.astype(BF16)
            self.total[...] = short
            self.out[:, self.columns(env.group)] = short.astype(F32)

        if self.whole:
            last()
        else:
            pl.when(self.mine)(last)
        self.other_copy = self.send(self.total, self.from_other, (env.other, env.dom), self.mine)

    def place(self):
        def last():
            self.other_copy.wait_recv()
            self.out[:, self.columns(self.env.other)] = self.from_other[...].astype(F32)

        if self.whole:
            last()
        else:
            pl.when(self.mine)(last)


class Env:
    pass


def layer_kernel(shape, *refs):
    node_count, edge_count, width, domains, slots, side, layers, plan = shape
    planes = side * side
    halo = domains * slots
    rows_all = node_count + halo
    inputs, refs = refs[:13], refs[13:]
    (edges_out, nodes_out, ein_out, eout_out, nin_out, nout_out, gain_out), refs = refs[:7], refs[7:]
    loaded, refs = refs[:13], refs[13:]
    (
        nodes, edges, ncot, ecot, send_row, recv_row, list_in, ein, eout, egain, nin, nout, ngain,
    ) = loaded
    (
        send_col, recv_col, list_col, outgoing, arrived, from_table, to_table, halo_table,
        even, odd, third, node_near, edge_slope, edge_act, edge_hat, edge_inv, edge_mid, edge_grad,
        gathered, node_act, node_mid, node_grad, gathered_grad, sums_from, sums_to, returning, returned,
        ein_grad, eout_grad, nin_grad, nout_grad,
        gains, gain_sum, gain_graph, gain_mine, gain_plane, gain_mid, gain_layer,
        load_sem, halo_sem, back_sem, gain_sem,
    ), refs = refs[:42], refs[42:]

    env = Env()
    env.group = lax.axis_index("group")
    env.dom = lax.axis_index("dom")
    env.other = 1 - env.group
    env.planes, env.layers, env.side = planes, layers, side
    env.layer = env.dom // planes
    env.plane = lax.rem(env.dom, planes)
    env.base = env.layer * planes
    x, y = lax.rem(env.plane, side), env.plane // side
    env.head, env.tail = x + env.group * (y - x), y + env.group * (x - y)
    env.head_stride = 1 + env.group * (side - 1)
    env.tail_stride = side - env.group * (side - 1)
    sent = []

    def send(src, dst, send_sem, recv_sem, device, when=None):
        copy = pltpu.make_async_remote_copy(
            src_ref=src, dst_ref=dst, send_sem=send_sem, recv_sem=recv_sem,
            device_id=device, device_id_type=MESH,
        )
        if when is None:
            copy.start()
        else:
            pl.when(when)(copy.start)
        sent.append((copy, when))
        return copy

    env.send = send

    def drain():
        for copy, when in sent:
            if when is None:
                copy.wait_send()
            else:
                pl.when(when)(copy.wait_send)
        sent.clear()

    def peer(step):
        return lax.rem(env.dom + step, domains)

    barrier = pltpu.get_barrier_semaphore()
    pl.semaphore_signal(barrier, inc=1, device_id=(env.other, env.dom), device_id_type=MESH)
    for step in range(1, domains):
        pl.semaphore_signal(barrier, inc=1, device_id=(env.group, peer(step)), device_id_type=MESH)

    loads = [
        pltpu.make_async_copy(src, dst, load_sem.at[index])
        for index, (src, dst) in enumerate(zip(inputs, loaded))
    ]
    NODES, EDGES, NCOT, ECOT, SEND, RECV, LIST, EIN, EOUT, EGAIN, NIN, NOUT, NGAIN = range(13)
    for index in (LIST, SEND, RECV, NODES, EIN, EDGES, EOUT, EGAIN, NIN, NOUT, NGAIN, NCOT, ECOT):
        loads[index].start()

    loads[LIST].wait()
    for index in range(domains):
        list_col[index * slots : (index + 1) * slots, :] = jnp.broadcast_to(
            list_in[:, index : index + 1], (slots, LANES)
        )
    loads[SEND].wait()
    loads[RECV].wait()

    for block in range(0, edge_count, LANES):
        place = slice(block, block + LANES)
        send_col[place, :] = jnp.transpose(jnp.broadcast_to(send_row[:, place], (LANES, LANES)))
        recv_col[place, :] = jnp.transpose(jnp.broadcast_to(recv_row[:, place], (LANES, LANES)))

    loads[NODES].wait()
    outgoing[...] = (
        dot(pick_rows(list_col[...], 0, node_count), nodes[...])
        .astype(BF16)
        .reshape(domains, slots, width)
    )
    pl.semaphore_wait(barrier, domains)
    halo_copies = [
        send(
            outgoing.at[peer(step)],
            arrived.at[env.dom],
            halo_sem.at[0, step - 1],
            halo_sem.at[1, step - 1],
            (env.group, peer(step)),
        )
        for step in range(1, domains)
    ]
    arrived[env.dom] = outgoing[env.dom]

    loads[EIN].wait()
    own_w = slice(0, width)
    from_w = slice(width, 2 * width)
    to_w = slice(2 * width, 3 * width)
    step_n = tile_of(node_count, (512, 256, 128))

    @pl.loop(0, node_count // step_n)
    def _(index):
        place = pl.ds(pl.multiple_of(index * step_n, step_n), step_n)
        from_table[place, :] = dot(nodes[place, :], ein[from_w, :]).astype(BF16)
        to_table[place, :] = dot(nodes[place, :], ein[to_w, :]).astype(BF16)

    for index in (EDGES, EOUT, EGAIN):
        loads[index].wait()
    step_e = even.shape[0]
    blocks = edge_count // step_e

    def tile(index):
        return slice(index * step_e, (index + 1) * step_e)

    buffers = (even, odd, third)

    def edge_lead(index, buffer):
        place = tile(index)
        buffer[...] = (
            dot(edges[place, :], ein[own_w, :])
            + dot(pick_rows(send_col[place, :], 0, node_count), from_table[...])
            + dot(pick_rows(recv_col[place, :], 0, node_count), to_table[...])
        )

    def halo_ready():
        for copy in halo_copies:
            copy.wait_recv()
        halo_table[...] = dot(arrived[...].reshape(halo, width), ein[from_w, :]).astype(BF16)

    def edge_follow(index, buffer):
        place = tile(index)
        value = buffer[...] + dot(
            pick_rows(send_col[place, :], node_count, halo), halo_table[...]
        )
        act, slope = swish_pair(value)
        act = act.astype(BF16)
        edge_act[place, :] = act
        edge_slope[place, :] = slope
        normed, inverse = normalize(dot(act, eout[...]))
        edge_hat[place, :] = normed
        edge_inv[place, :] = jnp.broadcast_to(inverse, (step_e, LANES))
        edge_mid[place, :] = (normed * egain[...]).astype(BF16)

    for index in range(3):
        edge_lead(index, buffers[index])
    loads[NIN].wait()
    near = slice(0, width)
    far = slice(width, 2 * width)
    node_near[...] = dot(nodes[...], nin[near, :])
    halo_ready()
    for index in range(blocks):
        edge_follow(index, buffers[index % 3])
        if index + 3 < blocks:
            edge_lead(index + 3, buffers[index % 3])

    for index in (NOUT, NGAIN, NCOT):
        loads[index].wait()
    gains[...] = jnp.zeros_like(gains)
    step_v = tile_of(node_count, (512, 256, 128))

    def collect(start):
        gathered[start : start + step_v, :] = dot(
            pick_columns(recv_row[...], start, step_v), edge_mid[...]
        ).astype(BF16)

    collect(0)
    for start in range(0, node_count, step_v):
        place = slice(start, start + step_v)
        if start + step_v < node_count:
            collect(start + step_v)
        act, slope = swish_pair(
            node_near[place, :] + dot(gathered[place, :], nin[far, :])
        )
        act = act.astype(BF16)
        node_act[place, :] = act
        normed, inverse = normalize(dot(act, nout[...]))
        upstream = ncot[place, :].astype(F32)
        gains[8:16, :] += fold(upstream * normed)
        post = norm_back(upstream, ngain[...], normed, inverse).astype(BF16)
        node_mid[place, :] = post
        grad = (dot_nt(post, nout[...]) * slope).astype(BF16)
        node_grad[place, :] = grad
        gathered_grad[place, :] = dot_nt(grad, nin[far, :]).astype(BF16)

    chunks = {}
    mats = {"ein": ein_grad, "eout": eout_grad, "nin": nin_grad, "nout": nout_grad}
    outs = {"ein": ein_out, "eout": eout_out, "nin": nin_out, "nout": nout_out}
    for index, (name, start, wide, begin, end) in enumerate(plan):
        chunks[name, start, begin] = Chunk(
            env, mats[name], outs[name], start, wide, begin, end, refs[index * 10 : (index + 1) * 10]
        )
    half = width // 2
    nout_c, nin_c, eout_c = (chunks[name, 0, 0] for name in ("nout", "nin", "eout"))
    low_c = (chunks["ein", 0, 0], chunks["ein", half, 0])
    high_c = (chunks["ein", 0, layers // 2], chunks["ein", half, layers // 2])

    nout_grad[...] = dot_tn(node_act[...], node_mid[...]).astype(BF16)
    nout_c.graph()
    nin_grad[near, :] = dot_tn(nodes[...], node_grad[...]).astype(BF16)
    nin_grad[far, :] = dot_tn(gathered[...], node_grad[...]).astype(BF16)

    loads[ECOT].wait()

    def back_lead(index, buffer):
        place = tile(index)
        buffer[...] = dot(pick_rows(recv_col[place, :], 0, node_count), gathered_grad[...])

    def back_follow(index, buffer):
        place = tile(index)
        upstream = ecot[place, :].astype(F32) + buffer[...]
        normed = edge_hat[place, :]
        gains[0:8, :] += fold(upstream * normed)
        post = norm_back(upstream, egain[...], normed, edge_inv[place, 0:1]).astype(BF16)
        edge_mid[place, :] = post
        edge_grad[place, :] = (dot_nt(post, eout[...]) * edge_slope[place, :]).astype(BF16)

    back_lead(0, buffers[0])
    nin_c.graph()
    for index in range(blocks):
        if index + 1 < blocks:
            back_lead(index + 1, buffers[(index + 1) % 2])
        back_follow(index, buffers[index % 2])
        if index == 0:
            nout_c.first()
            nin_c.first()

    step_s = tile_of(rows_all, (576, 512, 384, 256, 128))
    step_t = tile_of(node_count, (512, 256, 128))

    def scatter_from(columns):
        @pl.loop(0, rows_all // step_s)
        def _(index):
            start = pl.multiple_of(index * step_s, 64)
            sums_from[pl.ds(start, step_s), columns] = dot(
                pick_columns(send_row[...], start, step_s), edge_grad[:, columns]
            ).astype(BF16)

    def scatter_to(columns):
        @pl.loop(0, node_count // step_t)
        def _(index):
            start = pl.multiple_of(index * step_t, step_t)
            sums_to[pl.ds(start, step_t), columns] = dot(
                pick_columns(recv_row[...], start, step_t), edge_grad[:, columns]
            ).astype(BF16)

    def own_and_from(columns):
        ein_grad[own_w, columns] = dot_tn(edges[...], edge_grad[:, columns]).astype(BF16)
        ein_grad[from_w, columns] = (
            dot_tn(nodes[...], sums_from[0:node_count, columns])
            + dot_tn(arrived[...].reshape(halo, width), sums_from[node_count:rows_all, columns])
        ).astype(BF16)

    def toward(columns):
        ein_grad[to_w, columns] = dot_tn(nodes[...], sums_to[:, columns]).astype(BF16)

    first, second = slice(0, half), slice(half, width)
    eout_grad[...] = dot_tn(edge_act[...], edge_mid[...]).astype(BF16)
    eout_c.graph()
    gain_sum[0:1, :] = jnp.sum(gains[0:8, :], axis=0, keepdims=True)
    gain_sum[1:2, :] = jnp.sum(gains[8:16, :], axis=0, keepdims=True)
    gain_graph_copy = send(
        gain_sum, gain_graph, gain_sem.at[0, 0], gain_sem.at[1, 0], (env.other, env.dom)
    )
    nout_c.second()

    scatter_from(first)
    own_and_from(first)
    low_c[0].graph()
    eout_c.first()
    gain_graph_copy.wait_recv()
    gain_mine[...] = gain_sum[...] + gain_graph[...]
    gain_copies = [
        send(
            gain_mine, gain_plane.at[step - 1], gain_sem.at[0, step], gain_sem.at[1, step],
            (env.group, env.base + lax.rem(env.plane + step, planes)),
        )
        for step in range(1, planes)
    ]
    scatter_to(first)
    toward(first)
    high_c[0].graph()
    low_c[0].first()
    nin_c.second()

    scatter_from(second)
    returning[...] = (
        dot_nt(sums_from[node_count:rows_all, :], ein[from_w, :])
        .astype(BF16)
        .reshape(domains, slots, width)
    )
    back_copies = [
        send(
            returning.at[peer(step)],
            returned.at[env.dom],
            back_sem.at[0, step - 1],
            back_sem.at[1, step - 1],
            (env.group, peer(step)),
        )
        for step in range(1, domains)
    ]
    returned[env.dom] = returning[env.dom]
    high_c[0].first()
    nout_c.along()
    own_and_from(second)
    low_c[1].graph()
    eout_c.second()
    total = gain_mine[...]
    for step in range(1, planes):
        gain_copies[step - 1].wait_recv()
        total = total + gain_plane[step - 1]
    gain_mid[...] = total
    gain_copies = [
        send(
            gain_mid, gain_layer.at[step - 1],
            gain_sem.at[0, planes + step - 1], gain_sem.at[1, planes + step - 1],
            (env.group, lax.rem(env.layer + step, layers) * planes + env.plane),
        )
        for step in range(1, layers)
    ]
    scatter_to(second)
    toward(second)
    high_c[1].graph()
    low_c[1].first()
    low_c[0].second()
    nin_c.along()

    def edge_tail(begin, end):
        for index in range(begin, end):
            place = tile(index)
            edges_out[place, :] = (
                ecot[place, :].astype(F32) + dot_nt(edge_grad[place, :], ein[own_w, :])
            ).astype(BF16)

    def node_tail(start):
        place = slice(start, start + step_v)
        node_near[place, :] = (
            ncot[place, :].astype(F32)
            + dot_nt(node_grad[place, :], nin[near, :])
            + dot_nt(sums_from[place, :], ein[from_w, :])
            + dot_nt(sums_to[place, :], ein[to_w, :])
        )

    edge_tail(0, blocks)
    high_c[1].first()
    high_c[0].second()
    for start in range(0, node_count // 2, step_v):
        node_tail(start)
    eout_c.along()
    for start in range(node_count // 2, node_count, step_v):
        node_tail(start)
    low_c[0].along()
    low_c[1].second()

    for step in range(1, domains):
        back_copies[step - 1].wait_recv()
    list_row = jnp.concatenate(
        [
            jnp.transpose(list_col[block : block + LANES, :])[0:1, :]
            for block in range(0, halo, LANES)
        ],
        axis=1,
    )
    back = returned[...].reshape(halo, width)
    for start in range(0, node_count, step_v):
        place = slice(start, start + step_v)
        nodes_out[place, :] = (
            node_near[place, :] + dot(pick_columns(list_row, start, step_v), back)
        ).astype(BF16)

    high_c[1].second()
    high_c[0].along()
    low_c[1].along()
    high_c[1].along()
    nout_c.finish()
    nin_c.finish()
    total = gain_mid[...]
    for step in range(1, layers):
        gain_copies[step - 1].wait_recv()
        total = total + gain_layer[step - 1]
    share = width // domains
    gain_out[...] = pltpu.roll(total, lax.rem(width - env.dom * share, width), 1)
    eout_c.finish()
    nout_c.place()
    low_c[0].finish()
    nin_c.place()
    high_c[0].finish()
    eout_c.place()
    low_c[1].finish()
    low_c[0].place()
    high_c[0].place()
    high_c[1].finish()
    low_c[1].place()
    high_c[1].place()
    drain()


def layer(args, domains, side, layers):
    planes = side * side
    nodes, edges, ncot, ecot, senders, receivers, lists, ein, eout, egain, nin, nout, ngain = args
    node_count, width = nodes.shape
    edge_count = edges.shape[0]
    slots = lists.shape[0]
    halo = domains * slots
    half = width // 2
    tile = tile_of(edge_count // 4, (512, 256, 128))
    plan = (
        ("nout", 0, half, 0, layers),
        ("nin", 0, half, 0, layers),
        ("eout", 0, half, 0, layers),
        ("ein", 0, half // 2, 0, layers // 2),
        ("ein", 0, half // 2, layers // 2, layers),
        ("ein", half, half // 2, 0, layers // 2),
        ("ein", half, half // 2, layers // 2, layers),
    )
    rows = {"ein": 3 * width, "eout": width, "nin": 2 * width, "nout": width}
    dma = pltpu.SemaphoreType.DMA
    vmem = pltpu.VMEM
    anywhere = pl.BlockSpec(memory_space=pl.ANY)
    inside = pl.BlockSpec(memory_space=pltpu.VMEM)
    share = {name: count // domains for name, count in rows.items()}
    out_shape = (
        vmem((edge_count, width), BF16),
        vmem((node_count, width), BF16),
        vmem((share["ein"], width), F32),
        vmem((share["eout"], width), F32),
        vmem((share["nin"], width), F32),
        vmem((share["nout"], width), F32),
        vmem((2, width), F32),
    )
    scratch = [vmem(arg.shape, arg.dtype) for arg in args]
    scratch += [
        vmem((edge_count, LANES), I32),
        vmem((edge_count, LANES), I32),
        vmem((halo, LANES), I32),
        vmem((domains, slots, width), BF16),
        vmem((domains, slots, width), BF16),
        vmem((node_count, width), BF16),
        vmem((node_count, width), BF16),
        vmem((halo, width), BF16),
        vmem((tile, width), F32),
        vmem((tile, width), F32),
        vmem((tile, width), F32),
        vmem((node_count, width), F32),
        vmem((edge_count, width), F32),
        vmem((edge_count, width), BF16),
        vmem((edge_count, width), F32),
        vmem((edge_count, LANES), F32),
        vmem((edge_count, width), BF16),
        vmem((edge_count, width), BF16),
        vmem((node_count, width), BF16),
        vmem((node_count, width), BF16),
        vmem((node_count, width), BF16),
        vmem((node_count, width), BF16),
        vmem((node_count, width), BF16),
        vmem((node_count + halo, width), BF16),
        vmem((node_count, width), BF16),
        vmem((domains, slots, width), BF16),
        vmem((domains, slots, width), BF16),
        vmem((3 * width, width), BF16),
        vmem((width, width), BF16),
        vmem((2 * width, width), BF16),
        vmem((width, width), BF16),
        vmem((16, width), F32),
        vmem((2, width), F32),
        vmem((2, width), F32),
        vmem((2, width), F32),
        vmem((planes - 1, 2, width), F32),
        vmem((2, width), F32),
        vmem((layers - 1, 2, width), F32),
        dma((13,)),
        dma((2, domains - 1)),
        dma((2, domains - 1)),
        dma((2, planes + layers - 1)),
    ]
    for name, _, wide, begin, end in plan:
        count = share[name]
        some = end - begin
        scratch += [
            vmem((some * planes * count, wide), BF16),
            vmem((side, side, some, count, wide), BF16),
            vmem((side - 1, side, some, count, wide), BF16),
            vmem((side, some, count, wide), BF16),
            vmem((side - 1, some, count, wide), BF16),
            vmem((some, count, wide), BF16),
            vmem((layers - 1, count, wide), BF16),
            vmem((count, wide), BF16),
            vmem((count, wide), BF16),
            dma((2, 2 * side + layers - 1)),
        ]
    shape = (node_count, edge_count, width, domains, slots, side, layers, plan)
    return pl.pallas_call(
        functools.partial(layer_kernel, shape),
        out_shape=out_shape,
        in_specs=[anywhere] * len(args),
        out_specs=(inside,) * len(out_shape),
        scratch_shapes=scratch,
        compiler_params=pltpu.CompilerParams(
            collective_id=0, has_side_effects=True, vmem_limit_bytes=56 * 1024 * 1024
        ),
        name="layer",
    )(*args)


def hand_kernel(*refs):
    sources, targets, shares, sems = refs[:7], refs[7:15], refs[15:17], refs[17]
    share = shares[0].shape[1]
    for row in range(2):
        shares[row][...] = sources[6][row : row + 1, 0:share]
    copies = [
        pltpu.make_async_copy(source, target, sems.at[index])
        for index, (source, target) in enumerate(zip(sources[:6] + shares, targets))
    ]
    for copy in copies:
        copy.start()
    for copy in copies:
        copy.wait()


def hand_out(results, share):
    inside = pl.BlockSpec(memory_space=pltpu.VMEM)
    anywhere = pl.BlockSpec(memory_space=pl.ANY)
    return pl.pallas_call(
        hand_kernel,
        out_shape=tuple(jax.ShapeDtypeStruct(value.shape, value.dtype) for value in results[:6])
        + (jax.ShapeDtypeStruct((1, share), F32),) * 2,
        in_specs=[inside] * 7,
        out_specs=(anywhere,) * 8,
        scratch_shapes=[pltpu.VMEM((1, share), F32), pltpu.VMEM((1, share), F32), pltpu.SemaphoreType.DMA((8,))],
        compiler_params=pltpu.CompilerParams(vmem_limit_bytes=6 * 1024 * 1024),
        name="hand_out",
    )(*results)


def local(
    nodes, edges, node_cotangent, edge_cotangent, senders, receivers, send_rows,
    edge_in, edge_out, edge_gain, node_in, node_out, node_gain,
):
    domains = lax.axis_size("dom")
    side = 1
    while 8 * side**3 <= domains:
        side *= 2
    width = nodes.shape[2]
    args = (
        nodes[0], edges[0], node_cotangent[0], edge_cotangent[0], senders, receivers,
        send_rows[0].T, edge_in, edge_out, edge_gain[None], node_in, node_out, node_gain[None],
    )
    results = layer(args, domains, side, domains // (side * side))
    results = hand_out(results, width // domains)
    grad_edges, grad_nodes, ein, eout, nin, nout, edge_share, node_share = results
    return grad_edges[None], grad_nodes[None], ein, eout, nin, nout, edge_share[0], node_share[0]


def solution(mesh):
    placed = (
        P("group", "dom", None),
        P("group", "dom", None),
        P("group", "dom", None),
        P("group", "dom", None),
        P("group", "dom"),
        P("group", "dom"),
        P("group", "dom", None),
        P(),
        P(),
        P(),
        P(),
        P(),
        P(),
    )
    return jax.shard_map(
        local,
        mesh=mesh,
        in_specs=placed,
        out_specs=(
            P("group", "dom", None),
            P("group", "dom", None),
            P("dom", None),
            P("dom", None),
            P("dom", None),
            P("dom", None),
            P("dom"),
            P("dom"),
        ),
        check_vma=False,
    )
```

```python
import functools

import jax
import jax.numpy as jnp
from jax import lax
from jax.experimental import pallas as pl
from jax.experimental.pallas import tpu as pltpu
from jax.sharding import PartitionSpec as P

MESH = pl.DeviceIdType.MESH
F32 = jnp.float32
BF16 = jnp.bfloat16
I32 = jnp.int32
LANES = 128


def dot(first, second):
    return jnp.dot(first, second, preferred_element_type=F32)


def dot_tn(first, second):
    return lax.dot_general(first, second, (((0,), (0,)), ((), ())), preferred_element_type=F32)


def dot_nt(first, second):
    return lax.dot_general(first, second, (((1,), (1,)), ((), ())), preferred_element_type=F32)


def normalize(hidden):
    centre = hidden - jnp.mean(hidden, axis=-1, keepdims=True)
    inverse = lax.rsqrt(jnp.mean(centre * centre, axis=-1, keepdims=True) + 1e-05)
    return centre * inverse, inverse


def norm_back(upstream, gain, normed, inverse):
    scaled = upstream * gain
    return inverse * (
        scaled
        - jnp.mean(scaled, axis=-1, keepdims=True)
        - normed * jnp.mean(scaled * normed, axis=-1, keepdims=True)
    )


def swish_pair(value):
    logistic = jax.nn.sigmoid(value)
    return value * logistic, logistic * (1.0 + value * (1.0 - logistic))


def hot(mask):
    return jnp.where(mask, 1.0, 0.0).astype(BF16)


def pick_rows(column, base, count):
    lane = lax.broadcasted_iota(I32, column.shape, 1)
    return jnp.concatenate(
        [hot(column == lane + (base + block)) for block in range(0, count, LANES)], axis=1
    )


def pick_columns(row, base, count):
    index = lax.broadcasted_iota(I32, (count, row.shape[1]), 0) + base
    return hot(index == row)


def fold(value):
    return jnp.sum(value.reshape(value.shape[0] // 8, 8, value.shape[1]), axis=0)


def tile_of(count, sizes):
    return next(size for size in sizes if count % size == 0)


class Chunk:
    def __init__(self, env, mat, out, start, wide, begin, end, refs):
        self.env, self.mat, self.out, self.start, self.wide = env, mat, out, start, wide
        self.begin, self.end = begin, end
        (
            self.from_graph, self.sum_graph, self.from_first, self.sum_first, self.from_second,
            self.sum_second, self.from_layer, self.total, self.from_other, self.sem,
        ) = refs
        self.slot = 0
        whole = begin == 0 and end == env.layers
        self.mine = None if whole else self.owned(env.layer)
        self.whole = whole
        first_row = begin * env.planes * self.total.shape[0]
        self.rows = slice(first_row, first_row + self.from_graph.shape[0])

    def owned(self, layer):
        return jnp.logical_and(layer >= self.begin, layer < self.end)

    def send(self, src, dst, device, when=None):
        slot = self.slot
        self.slot += 1
        return self.env.send(src, dst, self.sem.at[0, slot], self.sem.at[1, slot], device, when)

    def columns(self, group):
        return pl.ds(pl.multiple_of(self.start + group * self.wide, LANES), self.wide)

    def graph(self):
        env = self.env
        self.graph_copy = self.send(
            self.mat.at[self.rows, self.columns(env.other)], self.from_graph, (env.other, env.dom)
        )

    def first(self):
        env = self.env
        side = env.side
        count = self.total.shape[0]
        self.graph_copy.wait_recv()
        for index in range((self.end - self.begin) * side * side):
            x, y, layer = index % side, index // side % side, index // (side * side)
            rows = slice(index * count, (index + 1) * count)
            there = slice(self.rows.start + rows.start, self.rows.start + rows.stop)
            value = self.mat[there, self.columns(env.group)].astype(F32)
            value = value + self.from_graph[rows, :].astype(F32)
            self.sum_graph[x + env.group * (y - x), y + env.group * (x - y), layer] = value.astype(BF16)
        self.copies = []
        for step in range(1, side):
            target = lax.rem(env.head + step, side)
            self.copies.append(
                self.send(
                    self.sum_graph.at[target],
                    self.from_first.at[step - 1],
                    (env.group, env.base + target * env.head_stride + env.tail * env.tail_stride),
                )
            )

    def second(self):
        env = self.env
        value = self.sum_graph[env.head].astype(F32)
        for step in range(1, env.side):
            self.copies[step - 1].wait_recv()
            value = value + self.from_first[step - 1].astype(F32)
        self.sum_first[...] = value.astype(BF16)
        self.copies = []
        for step in range(1, env.side):
            target = lax.rem(env.tail + step, env.side)
            self.copies.append(
                self.send(
                    self.sum_first.at[target],
                    self.from_second.at[step - 1],
                    (env.group, env.base + env.head * env.head_stride + target * env.tail_stride),
                )
            )

    def along(self):
        env = self.env
        value = self.sum_first[env.tail].astype(F32)
        for step in range(1, env.side):
            self.copies[step - 1].wait_recv()
            value = value + self.from_second[step - 1].astype(F32)
        self.sum_second[...] = value.astype(BF16)
        self.copies = []
        for step in range(1, env.layers):
            target = lax.rem(env.layer + step, env.layers)
            place = target if self.whole else jnp.clip(target - self.begin, 0, self.end - self.begin - 1)
            self.copies.append(
                self.send(
                    self.sum_second.at[place],
                    self.from_layer.at[step - 1],
                    (env.group, target * env.planes + env.plane),
                    None if self.whole else self.owned(target),
                )
            )

    def finish(self):
        env = self.env

        def last():
            place = env.layer - self.begin
            if not self.whole:
                place = jnp.clip(place, 0, self.end - self.begin - 1)
            value = self.sum_second[place].astype(F32)
            for step in range(1, env.layers):
                self.copies[step - 1].wait_recv()
                value = value + self.from_layer[step - 1].astype(F32)
            short = value.astype(BF16)
            self.total[...] = short
            self.out[:, self.columns(env.group)] = short.astype(F32)

        if self.whole:
            last()
        else:
            pl.when(self.mine)(last)
        self.other_copy = self.send(self.total, self.from_other, (env.other, env.dom), self.mine)

    def place(self):
        def last():
            self.other_copy.wait_recv()
            self.out[:, self.columns(self.env.other)] = self.from_other[...].astype(F32)

        if self.whole:
            last()
        else:
            pl.when(self.mine)(last)


class Env:
    pass


def layer_kernel(shape, *refs):
    node_count, edge_count, width, domains, slots, side, layers, plan = shape
    planes = side * side
    halo = domains * slots
    rows_all = node_count + halo
    inputs, refs = refs[:13], refs[13:]
    (edges_out, nodes_out, ein_out, eout_out, nin_out, nout_out, gain_out), refs = refs[:7], refs[7:]
    loaded, refs = refs[:13], refs[13:]
    (
        nodes, edges, ncot, ecot, send_row, recv_row, list_in, ein, eout, egain, nin, nout, ngain,
    ) = loaded
    (
        send_col, recv_col, list_col, outgoing, arrived, from_table, to_table, halo_table,
        even, odd, third, node_near, edge_slope, edge_act, edge_hat, edge_inv, edge_mid, edge_grad,
        gathered, node_act, node_mid, node_grad, gathered_grad, sums_from, sums_to, returning, returned,
        ein_grad, eout_grad, nin_grad, nout_grad,
        gains, gain_sum, gain_graph, gain_mine, gain_plane, gain_mid, gain_layer,
        load_sem, halo_sem, back_sem, gain_sem,
    ), refs = refs[:42], refs[42:]

    env = Env()
    env.group = lax.axis_index("group")
    env.dom = lax.axis_index("dom")
    env.other = 1 - env.group
    env.planes, env.layers, env.side = planes, layers, side
    env.layer = env.dom // planes
    env.plane = lax.rem(env.dom, planes)
    env.base = env.layer * planes
    x, y = lax.rem(env.plane, side), env.plane // side
    env.head, env.tail = x + env.group * (y - x), y + env.group * (x - y)
    env.head_stride = 1 + env.group * (side - 1)
    env.tail_stride = side - env.group * (side - 1)
    sent = []

    def send(src, dst, send_sem, recv_sem, device, when=None):
        copy = pltpu.make_async_remote_copy(
            src_ref=src, dst_ref=dst, send_sem=send_sem, recv_sem=recv_sem,
            device_id=device, device_id_type=MESH,
        )
        if when is None:
            copy.start()
        else:
            pl.when(when)(copy.start)
        sent.append((copy, when))
        return copy

    env.send = send

    def drain():
        for copy, when in sent:
            if when is None:
                copy.wait_send()
            else:
                pl.when(when)(copy.wait_send)
        sent.clear()

    def peer(step):
        return lax.rem(env.dom + step, domains)

    barrier = pltpu.get_barrier_semaphore()
    pl.semaphore_signal(barrier, inc=1, device_id=(env.other, env.dom), device_id_type=MESH)
    for step in range(1, domains):
        pl.semaphore_signal(barrier, inc=1, device_id=(env.group, peer(step)), device_id_type=MESH)

    loads = [
        pltpu.make_async_copy(src, dst, load_sem.at[index])
        for index, (src, dst) in enumerate(zip(inputs, loaded))
    ]
    NODES, EDGES, NCOT, ECOT, SEND, RECV, LIST, EIN, EOUT, EGAIN, NIN, NOUT, NGAIN = range(13)
    for index in (LIST, SEND, RECV, NODES, EIN, EDGES, EOUT, EGAIN, NIN, NOUT, NGAIN, NCOT, ECOT):
        loads[index].start()

    loads[LIST].wait()
    for index in range(domains):
        list_col[index * slots : (index + 1) * slots, :] = jnp.broadcast_to(
            list_in[:, index : index + 1], (slots, LANES)
        )
    loads[SEND].wait()
    loads[RECV].wait()

    for block in range(0, edge_count, LANES):
        place = slice(block, block + LANES)
        send_col[place, :] = jnp.transpose(jnp.broadcast_to(send_row[:, place], (LANES, LANES)))
        recv_col[place, :] = jnp.transpose(jnp.broadcast_to(recv_row[:, place], (LANES, LANES)))

    loads[NODES].wait()
    outgoing[...] = (
        dot(pick_rows(list_col[...], 0, node_count), nodes[...])
        .astype(BF16)
        .reshape(domains, slots, width)
    )
    pl.semaphore_wait(barrier, domains)
    halo_copies = [
        send(
            outgoing.at[peer(step)],
            arrived.at[env.dom],
            halo_sem.at[0, step - 1],
            halo_sem.at[1, step - 1],
            (env.group, peer(step)),
        )
        for step in range(1, domains)
    ]
    arrived[env.dom] = outgoing[env.dom]

    loads[EIN].wait()
    own_w = slice(0, width)
    from_w = slice(width, 2 * width)
    to_w = slice(2 * width, 3 * width)
    step_n = tile_of(node_count, (512, 256, 128))

    for start in range(0, node_count, step_n):
        place = slice(start, start + step_n)
        from_table[place, :] = dot(nodes[place, :], ein[from_w, :]).astype(BF16)
        to_table[place, :] = dot(nodes[place, :], ein[to_w, :]).astype(BF16)

    for index in (EDGES, EOUT, EGAIN):
        loads[index].wait()
    step_e = even.shape[0]
    blocks = edge_count // step_e

    def tile(index):
        return slice(index * step_e, (index + 1) * step_e)

    buffers = (even, odd, third)

    def edge_lead(index, buffer):
        place = tile(index)
        buffer[...] = (
            dot(edges[place, :], ein[own_w, :])
            + dot(pick_rows(send_col[place, :], 0, node_count), from_table[...])
            + dot(pick_rows(recv_col[place, :], 0, node_count), to_table[...])
        )

    def halo_ready():
        for copy in halo_copies:
            copy.wait_recv()
        halo_table[...] = dot(arrived[...].reshape(halo, width), ein[from_w, :]).astype(BF16)

    def edge_follow(index, buffer):
        place = tile(index)
        value = buffer[...] + dot(
            pick_rows(send_col[place, :], node_count, halo), halo_table[...]
        )
        act, slope = swish_pair(value)
        act = act.astype(BF16)
        edge_act[place, :] = act
        edge_slope[place, :] = slope
        normed, inverse = normalize(dot(act, eout[...]))
        edge_hat[place, :] = normed
        edge_inv[place, :] = jnp.broadcast_to(inverse, (step_e, LANES))
        edge_mid[place, :] = (normed * egain[...]).astype(BF16)

    for index in range(3):
        edge_lead(index, buffers[index])
    loads[NIN].wait()
    near = slice(0, width)
    far = slice(width, 2 * width)
    node_near[...] = dot(nodes[...], nin[near, :])
    halo_ready()
    for index in range(blocks):
        edge_follow(index, buffers[index % 3])
        if index + 3 < blocks:
            edge_lead(index + 3, buffers[index % 3])

    for index in (NOUT, NGAIN, NCOT):
        loads[index].wait()
    gains[...] = jnp.zeros_like(gains)
    step_v = tile_of(node_count, (512, 256, 128))

    def collect(start):
        gathered[start : start + step_v, :] = dot(
            pick_columns(recv_row[...], start, step_v), edge_mid[...]
        ).astype(BF16)

    collect(0)
    for start in range(0, node_count, step_v):
        place = slice(start, start + step_v)
        if start + step_v < node_count:
            collect(start + step_v)
        act, slope = swish_pair(
            node_near[place, :] + dot(gathered[place, :], nin[far, :])
        )
        act = act.astype(BF16)
        node_act[place, :] = act
        normed, inverse = normalize(dot(act, nout[...]))
        upstream = ncot[place, :].astype(F32)
        gains[8:16, :] += fold(upstream * normed)
        post = norm_back(upstream, ngain[...], normed, inverse).astype(BF16)
        node_mid[place, :] = post
        grad = (dot_nt(post, nout[...]) * slope).astype(BF16)
        node_grad[place, :] = grad
        gathered_grad[place, :] = dot_nt(grad, nin[far, :]).astype(BF16)

    chunks = {}
    mats = {"ein": ein_grad, "eout": eout_grad, "nin": nin_grad, "nout": nout_grad}
    outs = {"ein": ein_out, "eout": eout_out, "nin": nin_out, "nout": nout_out}
    for index, (name, start, wide, begin, end) in enumerate(plan):
        chunks[name, start, begin] = Chunk(
            env, mats[name], outs[name], start, wide, begin, end, refs[index * 10 : (index + 1) * 10]
        )
    half = width // 2
    nout_c, nin_c, eout_c = (chunks[name, 0, 0] for name in ("nout", "nin", "eout"))
    low_c = (chunks["ein", 0, 0], chunks["ein", half, 0])
    high_c = (chunks["ein", 0, layers // 2], chunks["ein", half, layers // 2])

    nout_grad[...] = dot_tn(node_act[...], node_mid[...]).astype(BF16)
    nout_c.graph()
    nin_grad[near, :] = dot_tn(nodes[...], node_grad[...]).astype(BF16)
    nin_grad[far, :] = dot_tn(gathered[...], node_grad[...]).astype(BF16)

    loads[ECOT].wait()

    def back_lead(index, buffer):
        place = tile(index)
        buffer[...] = dot(pick_rows(recv_col[place, :], 0, node_count), gathered_grad[...])

    def back_follow(index, buffer):
        place = tile(index)
        upstream = ecot[place, :].astype(F32) + buffer[...]
        normed = edge_hat[place, :]
        gains[0:8, :] += fold(upstream * normed)
        post = norm_back(upstream, egain[...], normed, edge_inv[place, 0:1]).astype(BF16)
        edge_mid[place, :] = post
        edge_grad[place, :] = (dot_nt(post, eout[...]) * edge_slope[place, :]).astype(BF16)

    back_lead(0, buffers[0])
    nin_c.graph()
    for index in range(blocks):
        if index + 1 < blocks:
            back_lead(index + 1, buffers[(index + 1) % 2])
        back_follow(index, buffers[index % 2])
        if index == 0:
            nout_c.first()
            nin_c.first()

    step_s = tile_of(rows_all, (576, 512, 384, 256, 128))
    step_t = tile_of(node_count, (512, 256, 128))

    def scatter_from(columns):
        @pl.loop(0, rows_all // step_s)
        def _(index):
            start = pl.multiple_of(index * step_s, 64)
            sums_from[pl.ds(start, step_s), columns] = dot(
                pick_columns(send_row[...], start, step_s), edge_grad[:, columns]
            ).astype(BF16)

    def scatter_to(columns):
        @pl.loop(0, node_count // step_t)
        def _(index):
            start = pl.multiple_of(index * step_t, step_t)
            sums_to[pl.ds(start, step_t), columns] = dot(
                pick_columns(recv_row[...], start, step_t), edge_grad[:, columns]
            ).astype(BF16)

    def own_and_from(columns):
        ein_grad[own_w, columns] = dot_tn(edges[...], edge_grad[:, columns]).astype(BF16)
        ein_grad[from_w, columns] = (
            dot_tn(nodes[...], sums_from[0:node_count, columns])
            + dot_tn(arrived[...].reshape(halo, width), sums_from[node_count:rows_all, columns])
        ).astype(BF16)

    def toward(columns):
        ein_grad[to_w, columns] = dot_tn(nodes[...], sums_to[:, columns]).astype(BF16)

    first, second = slice(0, half), slice(half, width)
    eout_grad[...] = dot_tn(edge_act[...], edge_mid[...]).astype(BF16)
    eout_c.graph()
    gain_sum[0:1, :] = jnp.sum(gains[0:8, :], axis=0, keepdims=True)
    gain_sum[1:2, :] = jnp.sum(gains[8:16, :], axis=0, keepdims=True)
    gain_graph_copy = send(
        gain_sum, gain_graph, gain_sem.at[0, 0], gain_sem.at[1, 0], (env.other, env.dom)
    )
    nout_c.second()

    scatter_from(first)
    own_and_from(first)
    low_c[0].graph()
    eout_c.first()
    gain_graph_copy.wait_recv()
    gain_mine[...] = gain_sum[...] + gain_graph[...]
    gain_copies = [
        send(
            gain_mine, gain_plane.at[step - 1], gain_sem.at[0, step], gain_sem.at[1, step],
            (env.group, env.base + lax.rem(env.plane + step, planes)),
        )
        for step in range(1, planes)
    ]
    scatter_to(first)
    toward(first)
    high_c[0].graph()
    low_c[0].first()
    nin_c.second()

    scatter_from(second)
    returning[...] = (
        dot_nt(sums_from[node_count:rows_all, :], ein[from_w, :])
        .astype(BF16)
        .reshape(domains, slots, width)
    )
    back_copies = [
        send(
            returning.at[peer(step)],
            returned.at[env.dom],
            back_sem.at[0, step - 1],
            back_sem.at[1, step - 1],
            (env.group, peer(step)),
        )
        for step in range(1, domains)
    ]
    returned[env.dom] = returning[env.dom]
    high_c[0].first()
    nout_c.along()
    own_and_from(second)
    low_c[1].graph()
    eout_c.second()
    total = gain_mine[...]
    for step in range(1, planes):
        gain_copies[step - 1].wait_recv()
        total = total + gain_plane[step - 1]
    gain_mid[...] = total
    gain_copies = [
        send(
            gain_mid, gain_layer.at[step - 1],
            gain_sem.at[0, planes + step - 1], gain_sem.at[1, planes + step - 1],
            (env.group, lax.rem(env.layer + step, layers) * planes + env.plane),
        )
        for step in range(1, layers)
    ]
    scatter_to(second)
    toward(second)
    high_c[1].graph()
    low_c[1].first()
    low_c[0].second()
    nin_c.along()

    def edge_tail(begin, end):
        for index in range(begin, end):
            place = tile(index)
            edges_out[place, :] = (
                ecot[place, :].astype(F32) + dot_nt(edge_grad[place, :], ein[own_w, :])
            ).astype(BF16)

    def node_tail(start):
        place = slice(start, start + step_v)
        node_near[place, :] = (
            ncot[place, :].astype(F32)
            + dot_nt(node_grad[place, :], nin[near, :])
            + dot_nt(sums_from[place, :], ein[from_w, :])
            + dot_nt(sums_to[place, :], ein[to_w, :])
        )

    edge_tail(0, blocks)
    high_c[1].first()
    high_c[0].second()
    for start in range(0, node_count // 2, step_v):
        node_tail(start)
    eout_c.along()
    for start in range(node_count // 2, node_count, step_v):
        node_tail(start)
    low_c[0].along()
    low_c[1].second()

    for step in range(1, domains):
        back_copies[step - 1].wait_recv()
    list_row = jnp.concatenate(
        [
            jnp.transpose(list_col[block : block + LANES, :])[0:1, :]
            for block in range(0, halo, LANES)
        ],
        axis=1,
    )
    back = returned[...].reshape(halo, width)
    for start in range(0, node_count, step_v):
        place = slice(start, start + step_v)
        nodes_out[place, :] = (
            node_near[place, :] + dot(pick_columns(list_row, start, step_v), back)
        ).astype(BF16)

    high_c[1].second()
    high_c[0].along()
    low_c[1].along()
    high_c[1].along()
    nout_c.finish()
    nin_c.finish()
    total = gain_mid[...]
    for step in range(1, layers):
        gain_copies[step - 1].wait_recv()
        total = total + gain_layer[step - 1]
    share = width // domains
    gain_out[...] = pltpu.roll(total, lax.rem(width - env.dom * share, width), 1)
    eout_c.finish()
    nout_c.place()
    low_c[0].finish()
    nin_c.place()
    high_c[0].finish()
    eout_c.place()
    low_c[1].finish()
    low_c[0].place()
    high_c[0].place()
    high_c[1].finish()
    low_c[1].place()
    high_c[1].place()
    drain()


def layer(args, domains, side, layers):
    planes = side * side
    nodes, edges, ncot, ecot, senders, receivers, lists, ein, eout, egain, nin, nout, ngain = args
    node_count, width = nodes.shape
    edge_count = edges.shape[0]
    slots = lists.shape[0]
    halo = domains * slots
    half = width // 2
    tile = tile_of(edge_count // 4, (512, 256, 128))
    plan = (
        ("nout", 0, half, 0, layers),
        ("nin", 0, half, 0, layers),
        ("eout", 0, half, 0, layers),
        ("ein", 0, half // 2, 0, layers // 2),
        ("ein", 0, half // 2, layers // 2, layers),
        ("ein", half, half // 2, 0, layers // 2),
        ("ein", half, half // 2, layers // 2, layers),
    )
    rows = {"ein": 3 * width, "eout": width, "nin": 2 * width, "nout": width}
    dma = pltpu.SemaphoreType.DMA
    vmem = pltpu.VMEM
    anywhere = pl.BlockSpec(memory_space=pl.ANY)
    inside = pl.BlockSpec(memory_space=pltpu.VMEM)
    share = {name: count // domains for name, count in rows.items()}
    out_shape = (
        vmem((edge_count, width), BF16),
        vmem((node_count, width), BF16),
        vmem((share["ein"], width), F32),
        vmem((share["eout"], width), F32),
        vmem((share["nin"], width), F32),
        vmem((share["nout"], width), F32),
        vmem((2, width), F32),
    )
    scratch = [vmem(arg.shape, arg.dtype) for arg in args]
    scratch += [
        vmem((edge_count, LANES), I32),
        vmem((edge_count, LANES), I32),
        vmem((halo, LANES), I32),
        vmem((domains, slots, width), BF16),
        vmem((domains, slots, width), BF16),
        vmem((node_count, width), BF16),
        vmem((node_count, width), BF16),
        vmem((halo, width), BF16),
        vmem((tile, width), F32),
        vmem((tile, width), F32),
        vmem((tile, width), F32),
        vmem((node_count, width), F32),
        vmem((edge_count, width), F32),
        vmem((edge_count, width), BF16),
        vmem((edge_count, width), F32),
        vmem((edge_count, LANES), F32),
        vmem((edge_count, width), BF16),
        vmem((edge_count, width), BF16),
        vmem((node_count, width), BF16),
        vmem((node_count, width), BF16),
        vmem((node_count, width), BF16),
        vmem((node_count, width), BF16),
        vmem((node_count, width), BF16),
        vmem((node_count + halo, width), BF16),
        vmem((node_count, width), BF16),
        vmem((domains, slots, width), BF16),
        vmem((domains, slots, width), BF16),
        vmem((3 * width, width), BF16),
        vmem((width, width), BF16),
        vmem((2 * width, width), BF16),
        vmem((width, width), BF16),
        vmem((16, width), F32),
        vmem((2, width), F32),
        vmem((2, width), F32),
        vmem((2, width), F32),
        vmem((planes - 1, 2, width), F32),
        vmem((2, width), F32),
        vmem((layers - 1, 2, width), F32),
        dma((13,)),
        dma((2, domains - 1)),
        dma((2, domains - 1)),
        dma((2, planes + layers - 1)),
    ]
    for name, _, wide, begin, end in plan:
        count = share[name]
        some = end - begin
        scratch += [
            vmem((some * planes * count, wide), BF16),
            vmem((side, side, some, count, wide), BF16),
            vmem((side - 1, side, some, count, wide), BF16),
            vmem((side, some, count, wide), BF16),
            vmem((side - 1, some, count, wide), BF16),
            vmem((some, count, wide), BF16),
            vmem((layers - 1, count, wide), BF16),
            vmem((count, wide), BF16),
            vmem((count, wide), BF16),
            dma((2, 2 * side + layers - 1)),
        ]
    shape = (node_count, edge_count, width, domains, slots, side, layers, plan)
    return pl.pallas_call(
        functools.partial(layer_kernel, shape),
        out_shape=out_shape,
        in_specs=[anywhere] * len(args),
        out_specs=(inside,) * len(out_shape),
        scratch_shapes=scratch,
        compiler_params=pltpu.CompilerParams(
            collective_id=0, has_side_effects=True, vmem_limit_bytes=56 * 1024 * 1024
        ),
        name="layer",
    )(*args)


def hand_kernel(*refs):
    sources, targets, shares, sems = refs[:7], refs[7:15], refs[15:17], refs[17]
    share = shares[0].shape[1]
    for row in range(2):
        shares[row][...] = sources[6][row : row + 1, 0:share]
    copies = [
        pltpu.make_async_copy(source, target, sems.at[index])
        for index, (source, target) in enumerate(zip(sources[:6] + shares, targets))
    ]
    for copy in copies:
        copy.start()
    for copy in copies:
        copy.wait()


def hand_out(results, share):
    inside = pl.BlockSpec(memory_space=pltpu.VMEM)
    anywhere = pl.BlockSpec(memory_space=pl.ANY)
    return pl.pallas_call(
        hand_kernel,
        out_shape=tuple(jax.ShapeDtypeStruct(value.shape, value.dtype) for value in results[:6])
        + (jax.ShapeDtypeStruct((1, share), F32),) * 2,
        in_specs=[inside] * 7,
        out_specs=(anywhere,) * 8,
        scratch_shapes=[pltpu.VMEM((1, share), F32), pltpu.VMEM((1, share), F32), pltpu.SemaphoreType.DMA((8,))],
        compiler_params=pltpu.CompilerParams(vmem_limit_bytes=6 * 1024 * 1024),
        name="hand_out",
    )(*results)


def local(
    nodes, edges, node_cotangent, edge_cotangent, senders, receivers, send_rows,
    edge_in, edge_out, edge_gain, node_in, node_out, node_gain,
):
    domains = lax.axis_size("dom")
    side = 1
    while 8 * side**3 <= domains:
        side *= 2
    width = nodes.shape[2]
    args = (
        nodes[0], edges[0], node_cotangent[0], edge_cotangent[0], senders, receivers,
        send_rows[0].T, edge_in, edge_out, edge_gain[None], node_in, node_out, node_gain[None],
    )
    results = layer(args, domains, side, domains // (side * side))
    results = hand_out(results, width // domains)
    grad_edges, grad_nodes, ein, eout, nin, nout, edge_share, node_share = results
    return grad_edges[None], grad_nodes[None], ein, eout, nin, nout, edge_share[0], node_share[0]


def solution(mesh):
    placed = (
        P("group", "dom", None),
        P("group", "dom", None),
        P("group", "dom", None),
        P("group", "dom", None),
        P("group", "dom"),
        P("group", "dom"),
        P("group", "dom", None),
        P(),
        P(),
        P(),
        P(),
        P(),
        P(),
    )
    return jax.shard_map(
        local,
        mesh=mesh,
        in_specs=placed,
        out_specs=(
            P("group", "dom", None),
            P("group", "dom", None),
            P("dom", None),
            P("dom", None),
            P("dom", None),
            P("dom", None),
            P("dom"),
            P("dom"),
        ),
        check_vma=False,
    )
```
